32 devices in a mesh: gx: 4 (over y, x), gy: 8 (over z, core).
Axes of the slice: x: 2, y: 2, z: 4, core: 2. Of those that a mesh axis runs over, the one named last changes fastest.
Arguments:
- replay_deter: float32 [8192, 2048], P(('gx', 'gy')), may hold values from -1 to 1
- replay_stoch: int32 [8192, 32], P(('gx', 'gy')), may hold values from 0 to 31
- send_rows: int32 [1024, 8], P(('gx', 'gy')), may hold values from 0 to 255
- send_counts: int32 [32, 32], P(('gx', 'gy')), may hold values from 0 to 8, as said below
- actions: int32 [8192, 4], P(('gx', 'gy')), may hold values from 0 to 17
- samples: int32 [8192, 4, 32], P(('gx', 'gy')), may hold values from 0 to 31
- w_stoch: bfloat16 [1024, 6144], P('gy'), may hold values from -1 to 1
- w_deter: bfloat16 [4, 512, 1536], P(None, 'gy'), may hold values from -0.25 to 0.25
- act_table: bfloat16 [18, 6144], replicated, may hold values from -3 to 3
- w_prior: bfloat16 [2048, 1024], P('gy'), may hold values from -0.037353516 to 0.037353516
Outputs:
- imagined: bfloat16 [8192, 4, 2048], P(('gx', 'gy'))
- log_prob: float32 [8192, 4, 32], P(('gx', 'gy'))
The draws below stay inside these ranges and needn't reach their ends.
Inputs may be any that keep to these rules, and one draw needn't show every extreme that they name: `send_rows`: entries past a destination's count are unused. `send_counts`: each source's counts sum to exactly 128; every source sends 8 rows to some owner, and some owner receives 8 rows from every source.
All inputs are finite; a program needn't handle non-finite values.
Results may differ from the reference program's by a relative error of at most 0.0022.
Values may be sent and summed in bfloat16 or wider, within the bound.
No kernel may reach another device: no remote copies, remote signals or barrier semaphores. Data moves between devices by JAX's collectives and lax.ppermute only.
A program may use at most 128 MiB of HBM per device.

```python
import jax
import jax.numpy as jnp
from jax import lax

GROUPS = 32
CLASSES = 32
BLOCKS = 4
BLOCK_W = 512
DETER = 2048
ACTIONS = 18
STEPS = 4
LENGTH = 64
SEQ_DEV = 4
SLOTS = 256
CAP = 8
LIVE = 128
DEVICES = 32


def draw_send_counts(key, part):
    frequent_choices = jax.random.randint(jax.random.fold_in(key, 11), (DEVICES,), 0, 6144)
    gumbel_jitter = jax.random.randint(jax.random.fold_in(key, 12), (DEVICES, DEVICES, CAP), 0, 4096)
    preference_boost = jax.random.randint(jax.random.fold_in(key, 13), (DEVICES,), 0, DEVICES)
    overfull_slots = jax.random.randint(jax.random.fold_in(key, 14), (), 0, DEVICES)
    owning_devices = jnp.arange(DEVICES, dtype=jnp.int32)
    extra_reward = jnp.where(owning_devices[None, :] == preference_boost[:, None], 16384, 0) + jnp.where(owning_devices[None, :] == overfull_slots, 12288, 0)
    ranking_score = gumbel_jitter + frequent_choices[None, :, None] + extra_reward[:, :, None]
    width = DEVICES * CAP
    keyed = ranking_score.reshape(DEVICES, width) * width + jnp.arange(width, dtype=jnp.int32)[None, :]
    best, chosen = lax.top_k(keyed, LIVE)
    picked = jnp.zeros((DEVICES, width), jnp.int32).at[jnp.arange(DEVICES)[:, None], chosen].set(1)
    return picked.reshape(DEVICES, DEVICES, CAP).sum(-1).astype(jnp.int32)


def with_ends(drawn, stream_key, low, high):
    index_at = [jax.random.randint(jax.random.fold_in(stream_key, axis), (), 0, length) for axis, length in enumerate(drawn.shape)]
    main_axis = drawn.shape.index(max(drawn.shape))
    next_to = index_at[:main_axis] + [(index_at[main_axis] + 1) % drawn.shape[main_axis]] + index_at[main_axis + 1:]
    return drawn.at[tuple(index_at)].set(low).at[tuple(next_to)].set(high)


def shard_levels(own_key, dims, pieces, least, high):
    level, own = 1.0, jax.random.fold_in(own_key, 6)
    for dim, parts in pieces:
        heights = jnp.exp(jax.random.uniform(jax.random.fold_in(own, dim), (parts,), jnp.float32, least / len(pieces), high / len(pieces)))
        level = level * jnp.repeat(heights, dims[dim] // parts).reshape([-1 if axis == dim else 1 for axis in range(len(dims))])
    return level


def centred(own_key, shape, deviation, limit, pieces=(), kind=jnp.bfloat16):
    gain = shard_levels(own_key, shape, pieces, -0.22, 0.18) if pieces else 1.0
    array = jax.random.normal(own_key, shape, jnp.float32) * deviation * gain
    return jnp.minimum(jnp.maximum(array, -limit), limit).astype(kind)


def setup_inputs(seed: int = 0) -> dict:
    keys = jax.random.split(jax.random.key(seed), 11)
    return {
        "replay_deter": jnp.clip(jax.random.uniform(keys[0], (DEVICES * SEQ_DEV * LENGTH, DETER), jnp.float32, -1.0, 1.0) * shard_levels(keys[0], (DEVICES * SEQ_DEV * LENGTH, DETER), ((0, 32),), -0.4, 0.0), -1.0, 1.0),
        "replay_stoch": with_ends(jax.random.randint(keys[1], (DEVICES * SEQ_DEV * LENGTH, GROUPS), 0, CLASSES), jax.random.fold_in(keys[1], 1), 0, CLASSES - 1).astype(jnp.int32),
        "send_rows": with_ends(jax.random.randint(keys[2], (DEVICES * DEVICES, CAP), 0, SEQ_DEV * LENGTH), jax.random.fold_in(keys[2], 1), 0, (SEQ_DEV * LENGTH) - 1).astype(jnp.int32),
        "send_counts": draw_send_counts(jax.random.fold_in(keys[10], 71), 0),
        "actions": with_ends(jax.random.randint(keys[4], (DEVICES * SLOTS, STEPS), 0, ACTIONS), jax.random.fold_in(keys[4], 1), 0, ACTIONS - 1).astype(jnp.int32),
        "samples": with_ends(jax.random.randint(keys[5], (DEVICES * SLOTS, STEPS, GROUPS), 0, CLASSES), jax.random.fold_in(keys[5], 1), 0, CLASSES - 1).astype(jnp.int32),
        "w_stoch": centred(keys[6], (GROUPS * CLASSES, 3 * DETER), GROUPS ** -0.5, 1.0, ((0, 8),)),
        "w_deter": centred(keys[7], (BLOCKS, BLOCK_W, 3 * BLOCK_W), BLOCK_W ** -0.5, 0.25, ((1, 8),)),
        "act_table": centred(keys[8], (ACTIONS, 3 * DETER), 0.5, 3.0),
        "w_prior": jnp.clip(jax.random.uniform(keys[9], (DETER, GROUPS * CLASSES), jnp.float32, -0.037353516, 0.037353516) * shard_levels(keys[9], (DETER, GROUPS * CLASSES), ((0, 8),), -0.4, 0.0), -0.037353516, 0.037353516).astype(jnp.bfloat16),
    }


def gru_step(state, stoch, action, w_stoch, w_deter, act_table):
    rows = state.shape[0]
    state_low = state.astype(jnp.bfloat16)
    onehot = (stoch[:, :, None] == jnp.arange(CLASSES, dtype=jnp.int32)[None, None, :]).reshape(rows, GROUPS * CLASSES).astype(jnp.bfloat16)
    act_hot = (action[:, None] == jnp.arange(ACTIONS, dtype=jnp.int32)[None, :]).astype(jnp.bfloat16)
    gates = jnp.dot(onehot, w_stoch, preferred_element_type=jnp.float32) + jnp.dot(act_hot, act_table, preferred_element_type=jnp.float32)
    gates = gates.reshape(rows, BLOCKS, 3 * BLOCK_W)
    blocked = state_low.reshape(rows, BLOCKS, BLOCK_W).astype(jnp.float32)
    gates = gates + jnp.einsum("rbi,bio->rbo", blocked, w_deter.astype(jnp.float32))
    reset = jax.nn.sigmoid(gates[..., :BLOCK_W])
    cand = jnp.tanh(reset * gates[..., BLOCK_W:2 * BLOCK_W])
    update = jax.nn.sigmoid(gates[..., 2 * BLOCK_W:] - 1.0)
    before = state.reshape(rows, BLOCKS, BLOCK_W)
    return (update * cand + (1.0 - update) * before).reshape(rows, BLOCKS * BLOCK_W)


def imagine(start, first, acts, samps, w_stoch, w_deter, act_table):
    state = start
    stoch = first
    states = []
    for step in range(STEPS):
        state = gru_step(state, stoch, acts[:, step], w_stoch, w_deter, act_table)
        states.append(state.astype(jnp.bfloat16))
        stoch = samps[:, step]
    return jnp.stack(states, 1)


def prior_logp(states, samps, w_prior):
    rows = states.shape[0]
    logits = jnp.dot(states.reshape(rows * STEPS, DETER), w_prior, preferred_element_type=jnp.float32)
    logits = logits.reshape(rows, STEPS, GROUPS, CLASSES)
    totals = jnp.log(jnp.sum(jnp.exp(logits), -1))
    hits = samps[..., None] == jnp.arange(CLASSES, dtype=jnp.int32)
    picked = jnp.sum(jnp.where(hits, logits, jnp.zeros_like(logits)), -1)
    return picked - totals


def reference(replay_deter, replay_stoch, send_rows, send_counts, actions, samples, w_stoch, w_deter, act_table, w_prior):
    count = DEVICES
    rows_dev = SEQ_DEV * LENGTH
    lists = send_rows.reshape(count, count, CAP)
    offsets = (jnp.arange(count, dtype=jnp.int32) * rows_dev)[:, None, None]
    global_rows = jnp.transpose(lists + offsets, (1, 0, 2)).astype(jnp.int32)
    live = jnp.arange(CAP, dtype=jnp.int32)[None, None, :] < jnp.transpose(send_counts)[:, :, None]
    acts_all = actions.reshape(count, SLOTS, STEPS)
    samps_all = samples.reshape(count, SLOTS, STEPS, GROUPS)

    def one_owner(inputs):
        picks, mask, acts, samps = inputs
        picks = picks.reshape(SLOTS)
        mask = mask.reshape(SLOTS)
        start = replay_deter[picks]
        first = replay_stoch[picks]
        states = imagine(start, first, acts, samps, w_stoch, w_deter, act_table)
        states = jnp.where(mask[:, None, None], states, jnp.zeros_like(states))
        logp = prior_logp(states, samps, w_prior)
        logp = jnp.where(mask[:, None, None], logp, jnp.zeros_like(logp))
        return states, logp

    states, logp = lax.map(one_owner, (global_rows, live, acts_all, samps_all))
    return states.reshape(count * SLOTS, STEPS, DETER), logp.reshape(count * SLOTS, STEPS, GROUPS)
```

```python
import jax
import jax.numpy as jnp
from jax import lax
from jax.sharding import PartitionSpec as P

GROUPS = 32
CLASSES = 32
STEPS = 4


def swap_pairs(count, mask):
    return [(a, a ^ mask) for a in range(count)]


def ring_gather(shard, count, index):
    chips = count // 2
    chip, core = index // 2, index % 2
    full = jnp.zeros((count,) + shard.shape, shard.dtype)
    piece = shard
    for hop in range(chips):
        if hop:
            piece = lax.ppermute(piece, "gy", [(a, (a + 2) % count) for a in range(count)])
        other = lax.ppermute(piece, "gy", swap_pairs(count, 1))
        place = lax.rem(chip + chips - hop, chips) * 2
        full = lax.dynamic_update_index_in_dim(full, piece, place + core, 0)
        full = lax.dynamic_update_index_in_dim(full, other, place + 1 - core, 0)
    return full


def one_hot(values, count):
    hot = values[..., None] == jnp.arange(count, dtype=jnp.int32)
    return hot.reshape(values.shape[0], -1).astype(jnp.bfloat16)


def make_on_device(nx, ny):
    def on_device(
        replay_deter,
        replay_stoch,
        send_rows,
        send_counts,
        actions,
        samples,
        w_stoch,
        w_deter,
        act_table,
        w_prior,
    ):
        peers, cap = send_rows.shape
        slots = peers * cap
        deter = replay_deter.shape[1]
        blocks = w_deter.shape[0]
        assert blocks == nx
        width = deter // blocks
        cols = 3 * width
        ix = lax.axis_index("gx")
        iy = lax.axis_index("gy")

        ws = lax.dynamic_slice_in_dim(w_stoch, ix * cols, cols, 1)
        wd = lax.dynamic_index_in_dim(w_deter, ix, 0, keepdims=False)
        wa = lax.dynamic_slice_in_dim(act_table, ix * cols, cols, 1)
        ws = ring_gather(ws, ny, iy).reshape(-1, cols)
        wd = ring_gather(wd, ny, iy).reshape(-1, cols)

        picks = send_rows.reshape(slots)
        start = replay_deter[picks].astype(jnp.float16).reshape(nx, ny, cap, blocks, width)
        mine = jnp.zeros((nx, ny, nx, cap, width), jnp.float16)
        for k in range(nx):
            part = lax.dynamic_index_in_dim(start, ix ^ k, 3, keepdims=False)
            if k:
                part = lax.ppermute(part, "gx", swap_pairs(nx, k))
            mine = lax.dynamic_update_index_in_dim(mine, part, ix ^ k, 2)
        rows = jnp.zeros((nx, nx, ny, cap, width), jnp.float16)
        for k in range(ny):
            part = lax.dynamic_index_in_dim(mine, iy ^ k, 1, keepdims=False)
            if k:
                part = lax.ppermute(part, "gy", swap_pairs(ny, k))
            rows = lax.dynamic_update_index_in_dim(rows, part, iy ^ k, 2)
        state = rows.reshape(nx * slots, width).astype(jnp.float32)

        first = replay_stoch[picks].reshape(nx, ny, cap * GROUPS)
        note = jnp.concatenate([first, send_counts[0].reshape(nx, ny, 1)], 2)
        note = jnp.transpose(note, (1, 0, 2)).astype(jnp.bfloat16)
        note = jnp.broadcast_to(note[None], (nx,) + note.shape).reshape(peers, nx, -1)
        note = lax.all_to_all(note, ("gx", "gy"), split_axis=0, concat_axis=0, tiled=True)
        note = note.astype(jnp.int32)
        first = jnp.transpose(note[:, :, : cap * GROUPS], (1, 0, 2)).reshape(nx * slots, GROUPS)
        counts = lax.dynamic_index_in_dim(note, ix, 1, keepdims=False)[:, cap * GROUPS]
        live = (jnp.arange(cap, dtype=jnp.int32)[None, :] < counts[:, None]).reshape(slots)

        known = jnp.concatenate([samples[:, : STEPS - 1].reshape(slots, -1), actions], 1)
        given = jnp.zeros((nx,) + known.shape, known.dtype)
        for k in range(nx):
            part = lax.ppermute(known, "gx", swap_pairs(nx, k)) if k else known
            given = lax.dynamic_update_index_in_dim(given, part, ix ^ k, 0)
        given = given.reshape(nx * slots, -1)

        wp = ring_gather(w_prior, ny, iy).reshape(deter, -1)

        log_prob = []
        states = []
        for step in range(STEPS):
            z = first if step == 0 else given[:, GROUPS * (step - 1) : GROUPS * step]
            act = given[:, GROUPS * (STEPS - 1) + step]
            gates = (
                jnp.dot(one_hot(z, CLASSES), ws, preferred_element_type=jnp.float32)
                + jnp.dot(
                    one_hot(act, act_table.shape[0]), wa, preferred_element_type=jnp.float32
                )
                + jnp.dot(state.astype(jnp.bfloat16), wd, preferred_element_type=jnp.float32)
            )
            reset = jax.nn.sigmoid(gates[:, :width])
            cand = jnp.tanh(reset * gates[:, width : 2 * width])
            update = jax.nn.sigmoid(gates[:, 2 * width :] - 1.0)
            state = update * cand + (1.0 - update) * state
            out = state.astype(jnp.bfloat16).reshape(nx, slots, width)
            whole = jnp.zeros((slots, deter), jnp.bfloat16)
            for k in range(nx):
                part = lax.dynamic_index_in_dim(out, ix ^ k, 0, keepdims=False)
                if k:
                    part = lax.ppermute(part, "gx", swap_pairs(nx, k))
                whole = lax.dynamic_update_slice_in_dim(whole, part, (ix ^ k) * width, 1)
            whole = jnp.where(live[:, None], whole, jnp.zeros_like(whole))
            states.append(whole)
            logits = jnp.dot(whole, wp, preferred_element_type=jnp.float32)
            logits = logits.reshape(slots, GROUPS, CLASSES)
            totals = jnp.log(jnp.sum(jnp.exp(logits), -1))
            hits = samples[:, step, :, None] == jnp.arange(CLASSES, dtype=jnp.int32)
            picked = jnp.sum(jnp.where(hits, logits, jnp.zeros_like(logits)), -1)
            log_prob.append(jnp.where(live[:, None], picked - totals, jnp.zeros_like(totals)))
        return (jnp.stack(states, 1), jnp.stack(log_prob, 1))

    return on_device


def solution(mesh):
    in_specs = (
        P(("gx", "gy"), None),
        P(("gx", "gy"), None),
        P(("gx", "gy"), None),
        P(("gx", "gy"), None),
        P(("gx", "gy"), None),
        P(("gx", "gy"), None, None),
        P("gy", None),
        P(None, "gy", None),
        P(),
        P("gy", None),
    )
    out_specs = (P(("gx", "gy"), None, None), P(("gx", "gy"), None, None))
    return jax.shard_map(
        make_on_device(mesh.shape["gx"], mesh.shape["gy"]),
        mesh=mesh,
        in_specs=in_specs,
        out_specs=out_specs,
        check_vma=False,
    )
```

```python
import functools
import jax
import jax.numpy as jnp
from jax import lax
from jax.experimental import pallas as pl
from jax.experimental.pallas import tpu as pltpu
from jax.sharding import PartitionSpec as P

GROUPS = 32
CLASSES = 32
STEPS = 4
BF16 = jnp.bfloat16
F32 = jnp.float32


def swap_pairs(count, mask):
    return [(a, a ^ mask) for a in range(count)]


def ring_pieces(shard, count):
    chips = count // 2
    piece = shard
    pieces = []
    for hop in range(chips):
        if hop:
            piece = lax.ppermute(piece, "gy", [(a, (a + 2) % count) for a in range(count)])
        pieces.append(piece)
        pieces.append(lax.ppermute(piece, "gy", swap_pairs(count, 1)))
    return pieces


def shard_of(chip, core, chips, n):
    return lax.rem(chip + chips - n // 2, chips) * 2 + (core ^ (n % 2))


def gru_kernel(chips, rows, cap, nx, idx, zt, act, x, mask, wa, *rest):
    pieces = rest[: 2 * chips]
    outs = rest[2 * chips : 2 * chips + nx]
    w_s, wd_s, oh_s, g_s, h_s, sems = rest[2 * chips + nx :]
    ix, chip, core = idx[0], idx[1], idx[2]
    srows = w_s.shape[0] // (2 * chips)
    drows = wd_s.shape[0] // (2 * chips)
    copies = []
    for n, piece in enumerate(pieces):
        place = shard_of(chip, core, chips, n)
        copies.append(
            pltpu.make_async_copy(
                piece.at[pl.ds(0, srows)],
                w_s.at[pl.ds(pl.multiple_of(place * srows, srows), srows)],
                sems.at[2 * n],
            )
        )
        copies.append(
            pltpu.make_async_copy(
                piece.at[pl.ds(srows, drows)],
                wd_s.at[pl.ds(pl.multiple_of(place * drows, drows), drows)],
                sems.at[2 * n + 1],
            )
        )
    for copy in copies:
        copy.start()
    width = wd_s.shape[0]
    kinds = w_s.shape[0]
    iota = lax.broadcasted_iota(jnp.int32, (CLASSES, rows), 0)
    for step in range(STEPS):
        for g in range(GROUPS):
            hot = jnp.broadcast_to(zt[step, g : g + 1, :], (CLASSES, rows)) == iota
            oh_s[g * CLASSES : (g + 1) * CLASSES, step * rows : (step + 1) * rows] = jnp.where(
                hot, 1.0, 0.0
            ).astype(BF16)
        hot = jnp.broadcast_to(act[step : step + 1, :], (CLASSES, rows)) == iota
        oh_s[kinds : kinds + CLASSES, step * rows : (step + 1) * rows] = jnp.where(
            hot, 1.0, 0.0
        ).astype(BF16)
    for k in range(nx):
        for l in range(2):
            for o in range(nx):
                place = (ix ^ o) * (nx * 2 * cap) + (ix ^ k) * (2 * cap) + (core ^ l) * cap
                h_s[pl.ds(pl.multiple_of(place, cap), cap), :] = x[
                    k * 2 + l, o * cap : (o + 1) * cap, :
                ]
    for copy in copies:
        copy.wait()
    dims = (((0,), (0,)), ((), ()))
    g_s[...] = lax.dot_general(
        oh_s[0:kinds, :], w_s[...], dims, preferred_element_type=F32
    ) + lax.dot_general(oh_s[kinds:, :], wa[...], dims, preferred_element_type=F32)
    keep = jnp.concatenate([mask[...]] * (width // 128), 1) > 0
    for step in range(STEPS):
        h = h_s[...]
        gates = g_s[step * rows : (step + 1) * rows, :] + jnp.dot(
            h.astype(BF16), wd_s[...], preferred_element_type=F32
        )
        reset = jax.nn.sigmoid(gates[:, :width])
        cand = jnp.tanh(reset * gates[:, width : 2 * width])
        update = jax.nn.sigmoid(gates[:, 2 * width :] - 1.0)
        h = update * cand + (1.0 - update) * h
        h_s[...] = h
        shown = jnp.where(keep, h, jnp.zeros_like(h)).astype(BF16)
        part = rows // nx
        for k in range(nx):
            outs[k][step] = shown[k * part : (k + 1) * part, :]


def prior_kernel(chips, nx, idx, zt, live, *rest):
    parts = rest[:nx]
    pieces = rest[nx : nx + 2 * chips]
    _, states, logp = rest[nx + 2 * chips : nx + 2 * chips + 3]
    wp_s, st_s, sems, out_sems = rest[nx + 2 * chips + 3 :]
    ix, chip, core, spot = idx[0], idx[1], idx[2], idx[3]
    prows = wp_s.shape[0] // (2 * chips)
    copies = []
    for n, piece in enumerate(pieces):
        place = shard_of(chip, core, chips, n)
        copies.append(
            pltpu.make_async_copy(
                piece, wp_s.at[pl.ds(pl.multiple_of(place * prows, prows), prows)], sems.at[n]
            )
        )
    for copy in copies:
        copy.start()
    width = parts[0].shape[2]
    count = parts[0].shape[1]
    for k in range(nx):
        at = pl.multiple_of((ix ^ k) * width, width)
        for step in range(STEPS):
            st_s[step, :, pl.ds(at, width)] = parts[k][step]
    outgo = []
    run = count // nx
    for step in range(STEPS):
        for a in range(nx):
            outgo.append(
                pltpu.make_async_copy(
                    st_s.at[step, pl.ds(a * run, run)],
                    states.at[step, a, spot],
                    out_sems.at[step * nx + a],
                )
            )
    for copy in outgo:
        copy.start()
    for copy in copies:
        copy.wait()
    logits = jnp.zeros((STEPS * count, wp_s.shape[1]), F32)
    for k in range(nx):
        at = pl.multiple_of((ix ^ k) * width, width)
        part = parts[k][...].reshape(STEPS * count, width)
        logits = logits + jnp.dot(part, wp_s[pl.ds(at, width), :], preferred_element_type=F32)
    turned = logits.T
    iota = lax.broadcasted_iota(jnp.int32, (CLASSES, STEPS * count), 0)
    for g in range(GROUPS):
        own = turned[g * CLASSES : (g + 1) * CLASSES, :]
        total = jnp.log(jnp.sum(jnp.exp(own), 0, keepdims=True))
        hot = jnp.broadcast_to(zt[g : g + 1, :], own.shape) == iota
        picked = jnp.sum(jnp.where(hot, own, jnp.zeros_like(own)), 0, keepdims=True)
        logp[g : g + 1, :] = jnp.where(live[0:1, :] > 0, picked - total, jnp.zeros_like(total))
    for copy in outgo:
        copy.wait()


VMEM = pl.BlockSpec(memory_space=pltpu.VMEM)
SMEM = pl.BlockSpec(memory_space=pltpu.SMEM)
ANY = pl.BlockSpec(memory_space=pl.ANY)


def fast_on_device(nx, ny):
    def on_device(
        replay_deter,
        replay_stoch,
        send_rows,
        send_counts,
        actions,
        samples,
        w_stoch,
        w_deter,
        act_table,
        w_prior,
    ):
        peers, cap = send_rows.shape
        slots = peers * cap
        deter = replay_deter.shape[1]
        blocks = w_deter.shape[0]
        width = deter // blocks
        cols = 3 * width
        chips = ny // 2
        part = nx * 2 * cap
        rows = nx * part
        ix = lax.axis_index("gx").astype(jnp.int32)
        iy = lax.axis_index("gy").astype(jnp.int32)
        chip, core = iy // 2, iy % 2
        near = jnp.arange(chips, dtype=jnp.int32) ^ chip
        across = jnp.arange(nx, dtype=jnp.int32) ^ ix

        ws = lax.dynamic_slice_in_dim(w_stoch, ix * cols, cols, 1)
        wd = lax.dynamic_index_in_dim(w_deter, ix, 0, keepdims=False)
        wa = lax.dynamic_slice_in_dim(act_table, ix * cols, cols, 1)
        wa = jnp.pad(wa, ((0, CLASSES - wa.shape[0]), (0, 0)))
        weights = ring_pieces(jnp.concatenate([ws, wd], 0), ny)

        dest = (
            jnp.arange(nx, dtype=jnp.int32)[None, None, :] * ny
            + near[None, :, None] * 2
            + (jnp.arange(2, dtype=jnp.int32) ^ core)[:, None, None]
        ).reshape(peers)
        picks = send_rows[dest].reshape(slots)
        start = replay_deter[picks].astype(jnp.float16)
        half = slots // 2
        held = []
        for k in range(nx):
            for l in range(2):
                piece = lax.dynamic_slice(
                    start, (l * half, (ix ^ k) * width), (half, width)
                )
                if k or l:
                    pairs = [
                        (a * ny + b, (a ^ k) * ny + (b ^ l)) for a in range(nx) for b in range(ny)
                    ]
                    piece = lax.ppermute(piece, ("gx", "gy"), pairs)
                held.append(piece)
        starts = []
        for m in range(chips):
            chunk = jnp.stack([p[m * nx * cap : (m + 1) * nx * cap] for p in held])
            if m:
                chunk = lax.ppermute(chunk, "gy", swap_pairs(ny, 2 * m))
            starts.append(chunk)

        first = replay_stoch[send_rows.reshape(slots)].reshape(nx, ny, cap * GROUPS)
        note = jnp.concatenate([first, send_counts[0].reshape(nx, ny, 1)], 2)
        note = jnp.transpose(note, (1, 0, 2)).astype(BF16)
        note = jnp.broadcast_to(note[None], (nx,) + note.shape).reshape(peers, nx, -1)
        note = lax.all_to_all(note, ("gx", "gy"), split_axis=0, concat_axis=0, tiled=True)
        note = note.astype(jnp.int32).reshape(nx, chips, 2, nx, -1)
        note = jnp.take(jnp.take(note, near, 1), across, 3)
        first = note[..., : cap * GROUPS].reshape(nx, chips, 2, nx, cap, GROUPS)
        first = jnp.transpose(first, (1, 5, 3, 0, 2, 4)).reshape(chips, GROUPS, rows)
        counts = jnp.transpose(note[..., cap * GROUPS], (1, 3, 0, 2))
        live = jnp.arange(cap, dtype=jnp.int32) < counts[..., None]
        live = live.reshape(chips, rows).astype(F32)
        masks = jnp.broadcast_to(live[:, :, None], (chips, rows, 128))
        lanes = jnp.tile(live[:, None, :part], (1, 8, STEPS))

        known = jnp.concatenate(
            [jnp.transpose(samples, (1, 2, 0)).reshape(-1, slots), jnp.transpose(actions)], 0
        )
        known = known.reshape(-1, nx, chips, 2 * cap)
        known = jnp.transpose(jnp.take(known, near, 2), (2, 0, 1, 3)).reshape(chips, -1, part)
        given = [known] + [lax.ppermute(known, "gx", swap_pairs(nx, k)) for k in range(1, nx)]
        given = jnp.concatenate(given, 2)
        tail = GROUPS * STEPS

        idx = jnp.stack([ix, chip, core, ix])
        priors = ring_pieces(w_prior, ny)

        parts = []
        for m in range(chips):
            zt = jnp.concatenate(
                [first[m], given[m, : GROUPS * (STEPS - 1)]], 0
            ).reshape(STEPS, GROUPS, rows)
            outs = pl.pallas_call(
                functools.partial(gru_kernel, chips, rows, cap, nx),
                out_shape=[jax.ShapeDtypeStruct((STEPS, part, width), BF16)] * nx,
                in_specs=[SMEM] + [VMEM] * 5 + [ANY] * (2 * chips),
                out_specs=[VMEM] * nx,
                scratch_shapes=[
                    pltpu.VMEM((GROUPS * CLASSES, cols), BF16),
                    pltpu.VMEM((width, cols), BF16),
                    pltpu.VMEM((GROUPS * CLASSES + CLASSES, STEPS * rows), BF16),
                    pltpu.VMEM((STEPS * rows, cols), F32),
                    pltpu.VMEM((rows, width), F32),
                    pltpu.SemaphoreType.DMA((4 * chips,)),
                ],
                compiler_params=pltpu.CompilerParams(vmem_limit_bytes=40 * 2**20),
                cost_estimate=pl.CostEstimate(
                    flops=2 * STEPS * rows * (1024 + 512) * cols,
                    transcendentals=0,
                    bytes_accessed=2 * 1536 * cols,
                ),
                name=f"gru_{m}",
            )(
                idx,
                zt,
                given[m, tail:],
                starts[m].astype(F32),
                masks[m],
                wa,
                *weights,
            )
            got = [outs[0]]
            for k in range(1, nx):
                got.append(lax.ppermute(outs[k], "gx", swap_pairs(nx, k)))
            parts.append(got)

        states = jnp.zeros((STEPS, nx, chips, 2 * cap, deter), BF16)
        logps = []
        for m in range(chips):
            zt = jnp.transpose(known[m, :tail].reshape(STEPS, GROUPS, part), (1, 0, 2))
            states, logp = pl.pallas_call(
                functools.partial(prior_kernel, chips, nx),
                out_shape=[
                    jax.ShapeDtypeStruct(states.shape, BF16),
                    jax.ShapeDtypeStruct((GROUPS, STEPS * part), F32),
                ],
                in_specs=[SMEM] + [VMEM] * (2 + nx) + [ANY] * (2 * chips) + [ANY],
                out_specs=[ANY, VMEM],
                input_output_aliases={3 + nx + 2 * chips: 0},
                scratch_shapes=[
                    pltpu.VMEM((deter, GROUPS * CLASSES), BF16),
                    pltpu.VMEM((STEPS, part, deter), BF16),
                    pltpu.SemaphoreType.DMA((2 * chips,)),
                    pltpu.SemaphoreType.DMA((STEPS * nx,)),
                ],
                compiler_params=pltpu.CompilerParams(vmem_limit_bytes=40 * 2**20),
                cost_estimate=pl.CostEstimate(
                    flops=2 * STEPS * part * deter * GROUPS * CLASSES,
                    transcendentals=0,
                    bytes_accessed=2 * deter * GROUPS * CLASSES,
                ),
                name=f"prior_{m}",
            )(
                jnp.stack([ix, chip, core, near[m]]),
                zt.reshape(GROUPS, STEPS * part),
                lanes[m],
                *parts[m],
                *priors,
                states,
            )
            logps.append(logp.reshape(GROUPS, STEPS, nx, 2 * cap))
        logp = jnp.take(jnp.stack(logps), near, 0)
        logp = jnp.transpose(logp, (3, 0, 4, 2, 1)).reshape(slots, STEPS, GROUPS)
        states = jnp.transpose(states.reshape(STEPS, slots, deter), (1, 0, 2))
        return (states, logp)

    return on_device

def ring_gather(shard, count, index):
    chips = count // 2
    chip, core = index // 2, index % 2
    full = jnp.zeros((count,) + shard.shape, shard.dtype)
    piece = shard
    for hop in range(chips):
        if hop:
            piece = lax.ppermute(piece, "gy", [(a, (a + 2) % count) for a in range(count)])
        other = lax.ppermute(piece, "gy", swap_pairs(count, 1))
        place = lax.rem(chip + chips - hop, chips) * 2
        full = lax.dynamic_update_index_in_dim(full, piece, place + core, 0)
        full = lax.dynamic_update_index_in_dim(full, other, place + 1 - core, 0)
    return full


def one_hot(values, count):
    hot = values[..., None] == jnp.arange(count, dtype=jnp.int32)
    return hot.reshape(values.shape[0], -1).astype(jnp.bfloat16)


def plain_on_device(nx, ny):
    def on_device(
        replay_deter,
        replay_stoch,
        send_rows,
        send_counts,
        actions,
        samples,
        w_stoch,
        w_deter,
        act_table,
        w_prior,
    ):
        peers, cap = send_rows.shape
        slots = peers * cap
        deter = replay_deter.shape[1]
        blocks = w_deter.shape[0]
        assert blocks == nx
        width = deter // blocks
        cols = 3 * width
        ix = lax.axis_index("gx")
        iy = lax.axis_index("gy")

        ws = lax.dynamic_slice_in_dim(w_stoch, ix * cols, cols, 1)
        wd = lax.dynamic_index_in_dim(w_deter, ix, 0, keepdims=False)
        wa = lax.dynamic_slice_in_dim(act_table, ix * cols, cols, 1)
        ws = ring_gather(ws, ny, iy).reshape(-1, cols)
        wd = ring_gather(wd, ny, iy).reshape(-1, cols)

        picks = send_rows.reshape(slots)
        start = replay_deter[picks].astype(jnp.float16).reshape(nx, ny, cap, blocks, width)
        mine = jnp.zeros((nx, ny, nx, cap, width), jnp.float16)
        for k in range(nx):
            part = lax.dynamic_index_in_dim(start, ix ^ k, 3, keepdims=False)
            if k:
                part = lax.ppermute(part, "gx", swap_pairs(nx, k))
            mine = lax.dynamic_update_index_in_dim(mine, part, ix ^ k, 2)
        rows = jnp.zeros((nx, nx, ny, cap, width), jnp.float16)
        for k in range(ny):
            part = lax.dynamic_index_in_dim(mine, iy ^ k, 1, keepdims=False)
            if k:
                part = lax.ppermute(part, "gy", swap_pairs(ny, k))
            rows = lax.dynamic_update_index_in_dim(rows, part, iy ^ k, 2)
        state = rows.reshape(nx * slots, width).astype(jnp.float32)

        first = replay_stoch[picks].reshape(nx, ny, cap * GROUPS)
        note = jnp.concatenate([first, send_counts[0].reshape(nx, ny, 1)], 2)
        note = jnp.transpose(note, (1, 0, 2)).astype(jnp.bfloat16)
        note = jnp.broadcast_to(note[None], (nx,) + note.shape).reshape(peers, nx, -1)
        note = lax.all_to_all(note, ("gx", "gy"), split_axis=0, concat_axis=0, tiled=True)
        note = note.astype(jnp.int32)
        first = jnp.transpose(note[:, :, : cap * GROUPS], (1, 0, 2)).reshape(nx * slots, GROUPS)
        counts = lax.dynamic_index_in_dim(note, ix, 1, keepdims=False)[:, cap * GROUPS]
        live = (jnp.arange(cap, dtype=jnp.int32)[None, :] < counts[:, None]).reshape(slots)

        known = jnp.concatenate([samples[:, : STEPS - 1].reshape(slots, -1), actions], 1)
        given = jnp.zeros((nx,) + known.shape, known.dtype)
        for k in range(nx):
            part = lax.ppermute(known, "gx", swap_pairs(nx, k)) if k else known
            given = lax.dynamic_update_index_in_dim(given, part, ix ^ k, 0)
        given = given.reshape(nx * slots, -1)

        wp = ring_gather(w_prior, ny, iy).reshape(deter, -1)

        log_prob = []
        states = []
        for step in range(STEPS):
            z = first if step == 0 else given[:, GROUPS * (step - 1) : GROUPS * step]
            act = given[:, GROUPS * (STEPS - 1) + step]
            gates = (
                jnp.dot(one_hot(z, CLASSES), ws, preferred_element_type=jnp.float32)
                + jnp.dot(
                    one_hot(act, act_table.shape[0]), wa, preferred_element_type=jnp.float32
                )
                + jnp.dot(state.astype(jnp.bfloat16), wd, preferred_element_type=jnp.float32)
            )
            reset = jax.nn.sigmoid(gates[:, :width])
            cand = jnp.tanh(reset * gates[:, width : 2 * width])
            update = jax.nn.sigmoid(gates[:, 2 * width :] - 1.0)
            state = update * cand + (1.0 - update) * state
            out = state.astype(jnp.bfloat16).reshape(nx, slots, width)
            whole = jnp.zeros((slots, deter), jnp.bfloat16)
            for k in range(nx):
                part = lax.dynamic_index_in_dim(out, ix ^ k, 0, keepdims=False)
                if k:
                    part = lax.ppermute(part, "gx", swap_pairs(nx, k))
                whole = lax.dynamic_update_slice_in_dim(whole, part, (ix ^ k) * width, 1)
            whole = jnp.where(live[:, None], whole, jnp.zeros_like(whole))
            states.append(whole)
            logits = jnp.dot(whole, wp, preferred_element_type=jnp.float32)
            logits = logits.reshape(slots, GROUPS, CLASSES)
            totals = jnp.log(jnp.sum(jnp.exp(logits), -1))
            hits = samples[:, step, :, None] == jnp.arange(CLASSES, dtype=jnp.int32)
            picked = jnp.sum(jnp.where(hits, logits, jnp.zeros_like(logits)), -1)
            log_prob.append(jnp.where(live[:, None], picked - totals, jnp.zeros_like(totals)))
        return (jnp.stack(states, 1), jnp.stack(log_prob, 1))

    return on_device


def solution(mesh):
    nx, ny = mesh.shape["gx"], mesh.shape["gy"]

    def on_device(*args):
        cap = args[2].shape[1]
        form = fast_on_device if cap % 8 == 0 else plain_on_device
        return form(nx, ny)(*args)

    in_specs = (
        P(("gx", "gy"), None),
        P(("gx", "gy"), None),
        P(("gx", "gy"), None),
        P(("gx", "gy"), None),
        P(("gx", "gy"), None),
        P(("gx", "gy"), None, None),
        P("gy", None),
        P(None, "gy", None),
        P(),
        P("gy", None),
    )
    out_specs = (P(("gx", "gy"), None, None), P(("gx", "gy"), None, None))
    return jax.shard_map(
        on_device, mesh=mesh, in_specs=in_specs, out_specs=out_specs, check_vma=False
    )
```

```python
import functools
import jax
import jax.numpy as jnp
from jax import lax
from jax.experimental import pallas as pl
from jax.experimental.pallas import tpu as pltpu
from jax.sharding import PartitionSpec as P


GROUPS = 32
CLASSES = 32
STEPS = 4
LANES = 128
SCALE = 32767.0
BF16 = jnp.bfloat16
F32 = jnp.float32
I32 = jnp.int32
I16 = jnp.int16


VMEM = pl.BlockSpec(memory_space=pltpu.VMEM)
SMEM = pl.BlockSpec(memory_space=pltpu.SMEM)
ANY = pl.BlockSpec(memory_space=pl.ANY)


def params(mib):
    return pltpu.CompilerParams(vmem_limit_bytes=mib * 2**20)


def swap_pairs(count, mask):
    return [(a, a ^ mask) for a in range(count)]


def tied(value, *others):
    return lax.optimization_barrier((value,) + others)[0]


def shard_of(chip, core, chips, n):
    return lax.rem(chip + chips - n // 2, chips) * 2 + (core ^ (n % 2))


def weights_kernel(idx, w_stoch, w_deter, out, sems):
    srows, cols = w_stoch.shape[0], out.shape[1]
    drows = w_deter.shape[1]
    at = pl.multiple_of(idx[0] * cols, cols)
    copies = [
        pltpu.make_async_copy(
            w_stoch.at[:, pl.ds(at, cols)], out.at[pl.ds(0, srows)], sems.at[0]
        ),
        pltpu.make_async_copy(w_deter.at[idx[0]], out.at[pl.ds(srows, drows)], sems.at[1]),
    ]
    for copy in copies:
        copy.start()
    for copy in copies:
        copy.wait()


def slot_map(chip, chips, run, shape, slot_dim):
    slot = lax.broadcasted_iota(I32, shape, slot_dim)
    place = lax.broadcasted_iota(I32, shape, 1 - slot_dim)
    part = shape[0] // chips
    chunk, rest = place // part, place % part
    return slot == ((rest // run) * chips + (chunk ^ chip)) * run + rest % run


def pack_kernel(chips, nx, cap, idx, rows_ref, counts, deter, stoch, samples, acts, *rest):
    outs = rest[: 2 * nx]
    known = rest[2 * nx]
    s_s, f_s = rest[2 * nx + 1 :]
    ix, chip, core = idx[0], idx[1], idx[2]
    slots = s_s.shape[0]
    half = slots // 2
    width = outs[0].shape[1] - LANES
    lane = lax.broadcasted_iota(I32, (1, LANES), 1)

    def one_dest(n, carry):
        l = n // (chips * nx)
        m = (n // nx) % chips
        o = n % nx
        dest = (o * chips + (m ^ chip)) * 2 + (l ^ core)
        count = counts[0, dest]
        for c in range(cap):
            src = rows_ref[dest, c]
            s_s[pl.ds(n * cap + c, 1), :] = deter[pl.ds(src, 1), :]
            flag = jnp.where(count > c, 1, 0)
            f_s[pl.ds(n * cap + c, 1), :] = jnp.where(
                lane == GROUPS, flag, stoch[pl.ds(src, 1), :]
            )
        return carry

    lax.fori_loop(0, slots // cap, one_dest, 0)
    for k in range(nx):
        at = pl.multiple_of((ix ^ k) * width, width)
        for l in range(2):
            part = s_s[l * half : (l + 1) * half, pl.ds(at, width)]
            out = outs[k * 2 + l]
            out[:, :width] = jnp.round(part * SCALE).astype(I32).astype(I16)
            out[:, width:] = f_s[l * half : (l + 1) * half, :].astype(I16)
    order = slot_map(chip, chips, 2 * cap, (slots, slots), 0)
    order = jnp.where(order, 1.0, 0.0).astype(BF16)
    tail = samples.shape[0]
    known[0:tail, :] = jnp.dot(
        samples[...].astype(F32).astype(BF16), order, preferred_element_type=F32
    ).astype(I32)
    known[tail:, :] = jnp.dot(
        acts[...].astype(F32).astype(BF16), order, preferred_element_type=F32
    ).astype(I32)


def fold_kernel(chips, run, *rest):
    pieces, outs = rest[:-chips], rest[-chips:]
    for m in range(chips):
        for n, piece in enumerate(pieces):
            outs[m][n] = piece[m * run : (m + 1) * run, :]


def place_kernel(chips, splits, idx, *rest):
    pieces, outs, sems = rest[: 2 * chips], rest[2 * chips : -1], rest[-1]
    copies = []
    for n, piece in enumerate(pieces):
        place = shard_of(idx[1], idx[2], chips, n)
        start = 0
        for o, run in enumerate(splits):
            copies.append(
                pltpu.make_async_copy(
                    piece.at[pl.ds(start, run)],
                    outs[o].at[pl.ds(pl.multiple_of(place * run, run), run)],
                    sems.at[n * len(splits) + o],
                )
            )
            start += run
    for copy in copies:
        copy.start()
    for copy in copies:
        copy.wait()


def gru_kernel(rows, cap, nx, m, idx, x, act_table, w_s, wd_s, *rest):
    given = rest[:nx]
    outs = rest[nx : 2 * nx]
    live, wa_s, oh_s, g_s, h_s, f_s, z_s = rest[2 * nx :]
    ix, core = idx[0], idx[2]
    width = wd_s.shape[0]
    kinds = w_s.shape[0]
    cols = w_s.shape[1]
    part = rows // nx
    wa_s[...] = jnp.zeros(wa_s.shape, BF16)
    wa_s[0 : act_table.shape[0], :] = act_table[:, pl.ds(pl.multiple_of(ix * cols, cols), cols)]
    for k in range(nx):
        for l in range(2):
            got = x[k * 2 + l].astype(I32).astype(F32)
            for o in range(nx):
                place = (ix ^ o) * part + (ix ^ k) * (2 * cap) + (core ^ l) * cap
                at = pl.ds(pl.multiple_of(place, cap), cap)
                h_s[at, :] = got[o * cap : (o + 1) * cap, :width] * (1.0 / SCALE)
                f_s[at, :] = got[o * cap : (o + 1) * cap, width:]
    turned = f_s[...].T
    live[...] = turned[GROUPS : GROUPS + 8, 0:part]
    tail = GROUPS * STEPS
    z_s[0:GROUPS, :] = turned[0:GROUPS, :].astype(I32)
    spot = slice(m * part, (m + 1) * part)
    z_s[GROUPS : GROUPS * STEPS, :] = jnp.concatenate(
        [g[0 : GROUPS * (STEPS - 1), spot] for g in given], 1
    )
    z_s[tail : tail + STEPS, :] = jnp.concatenate(
        [g[tail : tail + STEPS, spot] for g in given], 1
    )
    iota = lax.broadcasted_iota(I32, (CLASSES, rows), 0)
    for step in range(STEPS):
        for g in range(GROUPS + 1):
            row = step * GROUPS + g if g < GROUPS else tail + step
            hot = jnp.broadcast_to(z_s[row : row + 1, :], (CLASSES, rows)) == iota
            oh_s[g * CLASSES : (g + 1) * CLASSES, step * rows : (step + 1) * rows] = jnp.where(
                hot, 1.0, 0.0
            ).astype(BF16)
    dims = (((0,), (0,)), ((), ()))
    g_s[...] = lax.dot_general(
        oh_s[0:kinds, :], w_s[...], dims, preferred_element_type=F32
    ) + lax.dot_general(oh_s[kinds:, :], wa_s[...], dims, preferred_element_type=F32)
    keep = jnp.broadcast_to(f_s[:, GROUPS : GROUPS + 1], (rows, width)) > 0
    for step in range(STEPS):
        h = h_s[...]
        gates = g_s[step * rows : (step + 1) * rows, :] + jnp.dot(
            h.astype(BF16), wd_s[...], preferred_element_type=F32
        )
        reset = jax.nn.sigmoid(gates[:, :width])
        cand = jnp.tanh(reset * gates[:, width : 2 * width])
        update = jax.nn.sigmoid(gates[:, 2 * width :] - 1.0)
        h = update * cand + (1.0 - update) * h
        h_s[...] = h
        shown = jnp.where(keep, h, jnp.zeros_like(h)).astype(BF16)
        for k in range(nx):
            outs[k][step] = shown[k * part : (k + 1) * part, :]


def prior_kernel(nx, m, idx, known, live, wp_s, *rest):
    parts = rest[:nx]
    _, states, logp, st_s, out_sems = rest[nx:]
    ix, chip = idx[0], idx[1]
    width = parts[0].shape[2]
    count = parts[0].shape[1]
    for k in range(nx):
        at = pl.multiple_of((ix ^ k) * width, width)
        for step in range(STEPS):
            st_s[step, :, pl.ds(at, width)] = parts[k][step]
    outgo = []
    run = count // nx
    for step in range(STEPS):
        for a in range(nx):
            outgo.append(
                pltpu.make_async_copy(
                    st_s.at[step, pl.ds(a * run, run)],
                    states.at[step, a, chip ^ m],
                    out_sems.at[step * nx + a],
                )
            )
    for copy in outgo:
        copy.start()
    logits = jnp.zeros((STEPS * count, wp_s.shape[1]), F32)
    for k in range(nx):
        at = pl.multiple_of((ix ^ k) * width, width)
        part = parts[k][...].reshape(STEPS * count, width)
        logits = logits + jnp.dot(part, wp_s[pl.ds(at, width), :], preferred_element_type=F32)
    turned = logits.T
    spot = slice(m * count, (m + 1) * count)
    z = jnp.concatenate(
        [known[t * GROUPS : (t + 1) * GROUPS, spot] for t in range(STEPS)], 1
    )
    alive = jnp.concatenate([live[0:1, :]] * STEPS, 1) > 0
    iota = lax.broadcasted_iota(I32, (CLASSES, STEPS * count), 0)
    for g in range(GROUPS):
        own = turned[g * CLASSES : (g + 1) * CLASSES, :]
        total = jnp.log(jnp.sum(jnp.exp(own), 0, keepdims=True))
        hot = jnp.broadcast_to(z[g : g + 1, :], own.shape) == iota
        picked = jnp.sum(jnp.where(hot, own, jnp.zeros_like(own)), 0, keepdims=True)
        logp[g : g + 1, :] = jnp.where(alive, picked - total, jnp.zeros_like(total))
    for copy in outgo:
        copy.wait()


def order_kernel(chips, run, idx, *rest):
    logps, out = rest[:-1], rest[-1]
    slots = out.shape[2]
    part = slots // chips
    order = slot_map(idx[1], chips, run, (slots, slots), 1)
    order = jnp.where(order, 1.0, 0.0).astype(BF16)
    for step in range(STEPS):
        value = jnp.concatenate([p[:, step * part : (step + 1) * part] for p in logps], 1)
        total = jnp.zeros(value.shape, F32)
        for _ in range(3):
            piece = value.astype(BF16)
            total = total + jnp.dot(piece, order, preferred_element_type=F32)
            value = value - piece.astype(F32)
        out[step] = total


def fast_on_device(nx, ny):
    def on_device(
        replay_deter,
        replay_stoch,
        send_rows,
        send_counts,
        actions,
        samples,
        w_stoch,
        w_deter,
        act_table,
        w_prior,
    ):
        peers, cap = send_rows.shape
        slots = peers * cap
        deter = replay_deter.shape[1]
        blocks = w_deter.shape[0]
        width = deter // blocks
        cols = 3 * width
        chips = ny // 2
        part = nx * 2 * cap
        rows = nx * part
        lined = width + LANES
        ix = lax.axis_index("gx").astype(I32)
        iy = lax.axis_index("gy").astype(I32)
        idx = jnp.stack([ix, lax.shift_right_logical(iy, 1), iy & 1])
        ring = [(a, (a + 2) % ny) for a in range(ny)]
        partner = swap_pairs(ny, 1)

        def call(kernel, out_shape, ins, outs, scratch=(), mib=40, flops=0, **kwargs):
            def run(*args):
                return pl.pallas_call(
                    kernel,
                    out_shape=out_shape,
                    in_specs=ins,
                    out_specs=outs,
                    scratch_shapes=scratch,
                    compiler_params=params(mib),
                    cost_estimate=pl.CostEstimate(
                        flops=flops, transcendentals=0, bytes_accessed=2**20
                    ),
                    **kwargs,
                )(*args)

            return run

        srows, drows = w_stoch.shape[0], w_deter.shape[1]
        shard = call(
            weights_kernel,
            jax.ShapeDtypeStruct((srows + drows, cols), BF16),
            [SMEM, ANY, ANY],
            VMEM,
            [pltpu.SemaphoreType.DMA((2,))],
        )(idx, w_stoch, w_deter)
        stops = [shard]
        for _ in range(1, chips):
            stops.append(lax.ppermute(stops[-1], "gy", ring))
        pieces = []
        for piece in stops:
            pieces += [piece, lax.ppermute(piece, "gy", partner)]

        stoch = jnp.pad(replay_stoch, ((0, 0), (0, LANES - replay_stoch.shape[1])))
        samp = jnp.transpose(samples, (1, 2, 0)).reshape(-1, slots)
        *held, known = call(
            functools.partial(pack_kernel, chips, nx, cap),
            [jax.ShapeDtypeStruct((slots // 2, lined), I16)] * (2 * nx)
            + [jax.ShapeDtypeStruct((samp.shape[0] + STEPS, slots), I32)],
            [SMEM] * 3 + [VMEM] * 4,
            [VMEM] * (2 * nx + 1),
            [pltpu.VMEM((slots, deter), F32), pltpu.VMEM((slots, LANES), I32)],
        )(idx, send_rows, send_counts, replay_deter, stoch, samp, jnp.transpose(actions))
        for k in range(nx):
            for l in range(2):
                if k or l:
                    pairs = [
                        (a * ny + b, (a ^ k) * ny + (b ^ l)) for a in range(nx) for b in range(ny)
                    ]
                    n = k * 2 + l
                    held[n] = lax.ppermute(held[n], ("gx", "gy"), pairs)
        given = [known]
        for k in range(1, nx):
            given.append(lax.ppermute(known, "gx", swap_pairs(nx, k)))
        starts = call(
            functools.partial(fold_kernel, chips, nx * cap),
            [jax.ShapeDtypeStruct((2 * nx, nx * cap, lined), I16)] * chips,
            [VMEM] * (2 * nx),
            [VMEM] * chips,
        )(*held)
        starts = list(starts)
        for m in range(1, chips):
            starts[m] = lax.ppermute(starts[m], "gy", swap_pairs(ny, 2 * m))
        w_all, wd_all = call(
            functools.partial(place_kernel, chips, (srows, drows)),
            [
                jax.ShapeDtypeStruct((ny * srows, cols), BF16),
                jax.ShapeDtypeStruct((ny * drows, cols), BF16),
            ],
            [SMEM] + [ANY] * (2 * chips),
            [VMEM] * 2,
            [pltpu.SemaphoreType.DMA((4 * chips,))],
        )(idx, *pieces)

        parts = []
        for m in range(chips):
            *outs, live = call(
                functools.partial(gru_kernel, rows, cap, nx, m),
                [jax.ShapeDtypeStruct((STEPS, part, width), BF16)] * nx
                + [jax.ShapeDtypeStruct((8, part), F32)],
                [SMEM] + [VMEM] * (4 + nx),
                [VMEM] * (nx + 1),
                [
                    pltpu.VMEM((CLASSES, cols), BF16),
                    pltpu.VMEM((GROUPS * CLASSES + CLASSES, STEPS * rows), BF16),
                    pltpu.VMEM((STEPS * rows, cols), F32),
                    pltpu.VMEM((rows, width), F32),
                    pltpu.VMEM((rows, LANES), F32),
                    pltpu.VMEM((GROUPS * STEPS + 8, rows), I32),
                ],
                flops=2 * STEPS * rows * (GROUPS * CLASSES + width) * cols,
            )(idx, starts[m], act_table, w_all, wd_all, *given)
            got = [outs[0]]
            for k in range(1, nx):
                got.append(lax.ppermute(outs[k], "gx", swap_pairs(nx, k)))
            parts.append((live, got))

        piece = tied(w_prior, parts[0][0])
        pieces = []
        for m in range(chips):
            pieces += [piece, lax.ppermute(piece, "gy", partner)]
            if m + 1 < chips:
                piece = lax.ppermute(piece, "gy", ring)
        (wp_all,) = call(
            functools.partial(place_kernel, chips, (w_prior.shape[0],)),
            [jax.ShapeDtypeStruct((deter, GROUPS * CLASSES), BF16)],
            [SMEM] + [ANY] * (2 * chips),
            [VMEM],
            [pltpu.SemaphoreType.DMA((2 * chips,))],
        )(idx, *pieces)

        states = jnp.zeros((STEPS, nx, chips, 2 * cap, deter), BF16)
        logps = []
        for m in range(chips):
            live, got = parts[m]
            states, logp = call(
                functools.partial(prior_kernel, nx, m),
                [
                    jax.ShapeDtypeStruct(states.shape, BF16),
                    jax.ShapeDtypeStruct((GROUPS, STEPS * part), F32),
                ],
                [SMEM] + [VMEM] * (3 + nx) + [ANY],
                [ANY, VMEM],
                [
                    pltpu.VMEM((STEPS, part, deter), BF16),
                    pltpu.SemaphoreType.DMA((STEPS * nx,)),
                ],
                flops=2 * STEPS * part * deter * GROUPS * CLASSES,
                input_output_aliases={4 + nx: 0},
            )(idx, known, live, wp_all, *got, states)
            logps.append(logp)
        logp = call(
            functools.partial(order_kernel, chips, 2 * cap),
            jax.ShapeDtypeStruct((STEPS, GROUPS, slots), F32),
            [SMEM] + [VMEM] * chips,
            VMEM,
        )(idx, *logps)
        states = jnp.transpose(states.reshape(STEPS, slots, deter), (1, 0, 2))
        return (states, jnp.transpose(logp, (2, 0, 1)))

    return on_device


def ring_gather(shard, count, index):
    chips = count // 2
    chip, core = index // 2, index % 2
    full = jnp.zeros((count,) + shard.shape, shard.dtype)
    piece = shard
    for hop in range(chips):
        if hop:
            piece = lax.ppermute(piece, "gy", [(a, (a + 2) % count) for a in range(count)])
        other = lax.ppermute(piece, "gy", swap_pairs(count, 1))
        place = lax.rem(chip + chips - hop, chips) * 2
        full = lax.dynamic_update_index_in_dim(full, piece, place + core, 0)
        full = lax.dynamic_update_index_in_dim(full, other, place + 1 - core, 0)
    return full


def one_hot(values, count):
    hot = values[..., None] == jnp.arange(count, dtype=jnp.int32)
    return hot.reshape(values.shape[0], -1).astype(jnp.bfloat16)


def plain_on_device(nx, ny):
    def on_device(
        replay_deter,
        replay_stoch,
        send_rows,
        send_counts,
        actions,
        samples,
        w_stoch,
        w_deter,
        act_table,
        w_prior,
    ):
        peers, cap = send_rows.shape
        slots = peers * cap
        deter = replay_deter.shape[1]
        blocks = w_deter.shape[0]
        assert blocks == nx
        width = deter // blocks
        cols = 3 * width
        ix = lax.axis_index("gx")
        iy = lax.axis_index("gy")

        ws = lax.dynamic_slice_in_dim(w_stoch, ix * cols, cols, 1)
        wd = lax.dynamic_index_in_dim(w_deter, ix, 0, keepdims=False)
        wa = lax.dynamic_slice_in_dim(act_table, ix * cols, cols, 1)
        ws = ring_gather(ws, ny, iy).reshape(-1, cols)
        wd = ring_gather(wd, ny, iy).reshape(-1, cols)

        picks = send_rows.reshape(slots)
        start = replay_deter[picks].astype(jnp.float16).reshape(nx, ny, cap, blocks, width)
        mine = jnp.zeros((nx, ny, nx, cap, width), jnp.float16)
        for k in range(nx):
            part = lax.dynamic_index_in_dim(start, ix ^ k, 3, keepdims=False)
            if k:
                part = lax.ppermute(part, "gx", swap_pairs(nx, k))
            mine = lax.dynamic_update_index_in_dim(mine, part, ix ^ k, 2)
        rows = jnp.zeros((nx, nx, ny, cap, width), jnp.float16)
        for k in range(ny):
            part = lax.dynamic_index_in_dim(mine, iy ^ k, 1, keepdims=False)
            if k:
                part = lax.ppermute(part, "gy", swap_pairs(ny, k))
            rows = lax.dynamic_update_index_in_dim(rows, part, iy ^ k, 2)
        state = rows.reshape(nx * slots, width).astype(jnp.float32)

        first = replay_stoch[picks].reshape(nx, ny, cap * GROUPS)
        note = jnp.concatenate([first, send_counts[0].reshape(nx, ny, 1)], 2)
        note = jnp.transpose(note, (1, 0, 2)).astype(jnp.bfloat16)
        note = jnp.broadcast_to(note[None], (nx,) + note.shape).reshape(peers, nx, -1)
        note = lax.all_to_all(note, ("gx", "gy"), split_axis=0, concat_axis=0, tiled=True)
        note = note.astype(jnp.int32)
        first = jnp.transpose(note[:, :, : cap * GROUPS], (1, 0, 2)).reshape(nx * slots, GROUPS)
        counts = lax.dynamic_index_in_dim(note, ix, 1, keepdims=False)[:, cap * GROUPS]
        live = (jnp.arange(cap, dtype=jnp.int32)[None, :] < counts[:, None]).reshape(slots)

        known = jnp.concatenate([samples[:, : STEPS - 1].reshape(slots, -1), actions], 1)
        given = jnp.zeros((nx,) + known.shape, known.dtype)
        for k in range(nx):
            part = lax.ppermute(known, "gx", swap_pairs(nx, k)) if k else known
            given = lax.dynamic_update_index_in_dim(given, part, ix ^ k, 0)
        given = given.reshape(nx * slots, -1)

        wp = ring_gather(w_prior, ny, iy).reshape(deter, -1)

        log_prob = []
        states = []
        for step in range(STEPS):
            z = first if step == 0 else given[:, GROUPS * (step - 1) : GROUPS * step]
            act = given[:, GROUPS * (STEPS - 1) + step]
            gates = (
                jnp.dot(one_hot(z, CLASSES), ws, preferred_element_type=jnp.float32)
                + jnp.dot(
                    one_hot(act, act_table.shape[0]), wa, preferred_element_type=jnp.float32
                )
                + jnp.dot(state.astype(jnp.bfloat16), wd, preferred_element_type=jnp.float32)
            )
            reset = jax.nn.sigmoid(gates[:, :width])
            cand = jnp.tanh(reset * gates[:, width : 2 * width])
            update = jax.nn.sigmoid(gates[:, 2 * width :] - 1.0)
            state = update * cand + (1.0 - update) * state
            out = state.astype(jnp.bfloat16).reshape(nx, slots, width)
            whole = jnp.zeros((slots, deter), jnp.bfloat16)
            for k in range(nx):
                part = lax.dynamic_index_in_dim(out, ix ^ k, 0, keepdims=False)
                if k:
                    part = lax.ppermute(part, "gx", swap_pairs(nx, k))
                whole = lax.dynamic_update_slice_in_dim(whole, part, (ix ^ k) * width, 1)
            whole = jnp.where(live[:, None], whole, jnp.zeros_like(whole))
            states.append(whole)
            logits = jnp.dot(whole, wp, preferred_element_type=jnp.float32)
            logits = logits.reshape(slots, GROUPS, CLASSES)
            totals = jnp.log(jnp.sum(jnp.exp(logits), -1))
            hits = samples[:, step, :, None] == jnp.arange(CLASSES, dtype=jnp.int32)
            picked = jnp.sum(jnp.where(hits, logits, jnp.zeros_like(logits)), -1)
            log_prob.append(jnp.where(live[:, None], picked - totals, jnp.zeros_like(totals)))
        return (jnp.stack(states, 1), jnp.stack(log_prob, 1))

    return on_device


def solution(mesh):
    nx, ny = mesh.shape["gx"], mesh.shape["gy"]

    def on_device(*args):
        if args[2].shape[1] % 8 == 0 and ny == 8:
            return fast_on_device(nx, ny)(*args)
        return plain_on_device(nx, ny)(*args)

    in_specs = (
        P(("gx", "gy"), None),
        P(("gx", "gy"), None),
        P(("gx", "gy"), None),
        P(("gx", "gy"), None),
        P(("gx", "gy"), None),
        P(("gx", "gy"), None, None),
        P("gy", None),
        P(None, "gy", None),
        P(),
        P("gy", None),
    )
    out_specs = (P(("gx", "gy"), None, None), P(("gx", "gy"), None, None))
    return jax.shard_map(
        on_device, mesh=mesh, in_specs=in_specs, out_specs=out_specs, check_vma=False
    )
```

```python
import functools
import jax
import jax.numpy as jnp
from jax import lax
from jax.experimental import pallas as pl
from jax.experimental.pallas import tpu as pltpu
from jax.sharding import PartitionSpec as P


GROUPS = 32
CLASSES = 32
STEPS = 4
LANES = 128
SCALE = 32767.0
BF16 = jnp.bfloat16
F32 = jnp.float32
I32 = jnp.int32
I16 = jnp.int16


VMEM = pl.BlockSpec(memory_space=pltpu.VMEM)
SMEM = pl.BlockSpec(memory_space=pltpu.SMEM)
ANY = pl.BlockSpec(memory_space=pl.ANY)
HBM = pl.BlockSpec(memory_space=pltpu.HBM)


def params(mib):
    return pltpu.CompilerParams(vmem_limit_bytes=mib * 2**20)


def swap_pairs(count, mask):
    return [(a, a ^ mask) for a in range(count)]


def shard_of(chip, core, chips, n):
    return lax.rem(chip + chips - n // 2, chips) * 2 + (core ^ (n % 2))


def weights_kernel(idx, w_stoch, w_deter, w_prior, out, quarter, sems):
    srows, cols = w_stoch.shape[0], out.shape[1]
    drows = w_deter.shape[1]
    wide = quarter.shape[1]
    at = pl.multiple_of(idx[0] * cols, cols)
    copies = [
        pltpu.make_async_copy(
            w_stoch.at[:, pl.ds(at, cols)], out.at[pl.ds(0, srows)], sems.at[0]
        ),
        pltpu.make_async_copy(w_deter.at[idx[0]], out.at[pl.ds(srows, drows)], sems.at[1]),
        pltpu.make_async_copy(
            w_prior.at[:, pl.ds(pl.multiple_of(idx[0] * wide, wide), wide)], quarter, sems.at[2]
        ),
    ]
    for copy in copies:
        copy.start()
    for copy in copies:
        copy.wait()


def slot_map(chip, chips, run, shape, slot_dim):
    slot = lax.broadcasted_iota(I32, shape, slot_dim)
    place = lax.broadcasted_iota(I32, shape, 1 - slot_dim)
    part = shape[0] // chips
    chunk, rest = place // part, place % part
    return slot == ((rest // run) * chips + (chunk ^ chip)) * run + rest % run


def pack_kernel(chips, nx, cap, idx, rows_ref, counts, deter, stoch, samples, acts, *rest):
    outs = rest[: 2 * nx]
    known = rest[2 * nx]
    s_s, f_s, p_s = rest[2 * nx + 1 :]
    ix, chip, core = idx[0], idx[1], idx[2]
    slots = s_s.shape[0]
    half = slots // 2
    width = outs[0].shape[1] - LANES
    lane = lax.broadcasted_iota(I32, (1, LANES), 1)
    spot = lax.broadcasted_iota(I32, (1, deter.shape[0]), 1)

    def one_dest(n, carry):
        l = n // (chips * nx)
        m = (n // nx) % chips
        o = n % nx
        dest = (o * chips + (m ^ chip)) * 2 + (l ^ core)
        count = counts[0, dest]
        for c in range(cap):
            src = rows_ref[c, dest]
            s_s[pl.ds(n * cap + c, 1), :] = deter[pl.ds(src, 1), :]
            p_s[pl.ds(n * cap + c, 1), :] = jnp.where(spot == src, 1.0, 0.0)
            f_s[pl.ds(n * cap + c, 1), :] = jnp.where(
                lane == GROUPS, jnp.where(count > c, 1.0, 0.0), 0.0
            )
        return carry

    lax.fori_loop(0, slots // cap, one_dest, 0)
    f_s[:, 0 : stoch.shape[0]] = lax.dot_general(
        p_s[...].astype(BF16),
        stoch[...].astype(F32).astype(BF16),
        (((1,), (1,)), ((), ())),
        preferred_element_type=F32,
    )
    for k in range(nx):
        at = pl.multiple_of((ix ^ k) * width, width)
        for l in range(2):
            part = s_s[l * half : (l + 1) * half, pl.ds(at, width)]
            out = outs[k * 2 + l]
            out[:, :width] = jnp.round(part * SCALE).astype(I32).astype(I16)
            out[:, width:] = f_s[l * half : (l + 1) * half, :].astype(I32).astype(I16)
    order = slot_map(chip, chips, 2 * cap, (slots, slots), 0)
    order = jnp.where(order, 1.0, 0.0).astype(BF16)
    tail = samples.shape[0]
    known[0:tail, :] = jnp.dot(
        samples[...].astype(F32).astype(BF16), order, preferred_element_type=F32
    ).astype(I32)
    known[tail:, :] = jnp.dot(
        acts[...].astype(F32).astype(BF16), order, preferred_element_type=F32
    ).astype(I32)


def fold_kernel(chips, run, *rest):
    pieces, outs = rest[:-chips], rest[-chips:]
    for m in range(chips):
        for n, piece in enumerate(pieces):
            outs[m][n] = piece[m * run : (m + 1) * run, :]


def place_kernel(chips, splits, first, held, idx, *rest):
    count = len(splits)
    outs, sems = rest[-1 - count : -1], rest[-1]
    pieces = rest[: len(rest) - 1 - count - held]
    copies = []
    for n, piece in enumerate(pieces):
        place = shard_of(idx[1], idx[2], chips, n + first)
        start = 0
        for o, run in enumerate(splits):
            copies.append(
                pltpu.make_async_copy(
                    piece.at[pl.ds(start, run)],
                    outs[o].at[pl.ds(pl.multiple_of(place * run, run), run)],
                    sems.at[n * count + o],
                )
            )
            start += run
    for copy in copies:
        copy.start()
    for copy in copies:
        copy.wait()


def column_kernel(chips, run, idx, *rest):
    pieces, out = rest[:-1], rest[-1]
    for hop, piece in enumerate(pieces):
        place = lax.rem(idx[1] + chips - hop, chips) * run
        out[pl.ds(pl.multiple_of(place, run), run), :] = piece[...]


def prior_weights_kernel(chips, nx, run, idx, *rest):
    pieces, out = rest[:-1], rest[-1]
    wide = out.shape[1] // nx
    for n, piece in enumerate(pieces):
        at = pl.multiple_of((idx[0] ^ (n // 2)) * wide, wide)
        for z in range(chips):
            place = (z * 2 + (idx[2] ^ (n % 2))) * run
            out[pl.ds(pl.multiple_of(place, run), run), pl.ds(at, wide)] = piece[
                z * run : (z + 1) * run, :
            ]


def gru_kernel(rows, cap, nx, m, idx, x, act_table, w_s, wd_s, *rest):
    given = rest[:nx]
    outs = rest[nx : 2 * nx]
    live, wa_s, oh_s, g_s, h_s, f_s, z_s = rest[2 * nx :]
    ix, core = idx[0], idx[2]
    width = wd_s.shape[0]
    kinds = w_s.shape[0]
    cols = w_s.shape[1]
    part = rows // nx
    wa_s[...] = jnp.zeros(wa_s.shape, BF16)
    wa_s[0 : act_table.shape[0], :] = act_table[:, pl.ds(pl.multiple_of(ix * cols, cols), cols)]
    for k in range(nx):
        for l in range(2):
            got = x[k * 2 + l].astype(I32).astype(F32)
            for o in range(nx):
                place = (ix ^ o) * part + (ix ^ k) * (2 * cap) + (core ^ l) * cap
                at = pl.ds(pl.multiple_of(place, cap), cap)
                h_s[at, :] = got[o * cap : (o + 1) * cap, :width] * (1.0 / SCALE)
                f_s[at, :] = got[o * cap : (o + 1) * cap, width:]
    turned = f_s[...].T
    live[...] = turned[GROUPS : GROUPS + 8, 0:part]
    tail = GROUPS * STEPS
    z_s[0:GROUPS, :] = turned[0:GROUPS, :].astype(I32)
    spot = slice(m * part, (m + 1) * part)
    z_s[GROUPS : GROUPS * STEPS, :] = jnp.concatenate(
        [g[0 : GROUPS * (STEPS - 1), spot] for g in given], 1
    )
    z_s[tail : tail + STEPS, :] = jnp.concatenate(
        [g[tail : tail + STEPS, spot] for g in given], 1
    )
    iota = lax.broadcasted_iota(I32, (CLASSES, rows), 0)
    for step in range(STEPS):
        for g in range(GROUPS + 1):
            row = step * GROUPS + g if g < GROUPS else tail + step
            hot = jnp.broadcast_to(z_s[row : row + 1, :], (CLASSES, rows)) == iota
            oh_s[g * CLASSES : (g + 1) * CLASSES, step * rows : (step + 1) * rows] = jnp.where(
                hot, 1.0, 0.0
            ).astype(BF16)
    dims = (((0,), (0,)), ((), ()))
    g_s[...] = lax.dot_general(
        oh_s[0:kinds, :], w_s[...], dims, preferred_element_type=F32
    ) + lax.dot_general(oh_s[kinds:, :], wa_s[...], dims, preferred_element_type=F32)
    keep = jnp.broadcast_to(f_s[:, GROUPS : GROUPS + 1], (rows, width)) > 0
    for step in range(STEPS):
        h = h_s[...]
        gates = g_s[step * rows : (step + 1) * rows, :] + jnp.dot(
            h.astype(BF16), wd_s[...], preferred_element_type=F32
        )
        reset = jax.nn.sigmoid(gates[:, :width])
        cand = jnp.tanh(reset * gates[:, width : 2 * width])
        update = jax.nn.sigmoid(gates[:, 2 * width :] - 1.0)
        h = update * cand + (1.0 - update) * h
        h_s[...] = h
        shown = jnp.where(keep, h, jnp.zeros_like(h)).astype(BF16)
        for k in range(nx):
            outs[k][step] = shown[k * part : (k + 1) * part, :]


def prior_kernel(nx, m, idx, known, live, wp_s, *rest):
    parts = rest[:nx]
    states, logp, st_s, out_sems = rest[-4:]
    ix, chip = idx[0], idx[1]
    width = parts[0].shape[2]
    count = parts[0].shape[1]
    for k in range(nx):
        at = pl.multiple_of((ix ^ k) * width, width)
        st_s[:, :, pl.ds(at, width)] = jnp.transpose(parts[k][...], (1, 0, 2))
    outgo = []
    run = count // nx
    for a in range(nx):
        outgo.append(
            pltpu.make_async_copy(
                st_s.at[pl.ds(a * run, run)], states.at[a, chip ^ m], out_sems.at[a]
            )
        )
    for copy in outgo:
        copy.start()
    logits = jnp.zeros((STEPS * count, wp_s.shape[1]), F32)
    for k in range(nx):
        at = pl.multiple_of((ix ^ k) * width, width)
        part = parts[k][...].reshape(STEPS * count, width)
        logits = logits + jnp.dot(part, wp_s[pl.ds(at, width), :], preferred_element_type=F32)
    turned = logits.T
    spot = slice(m * count, (m + 1) * count)
    z = jnp.concatenate(
        [known[t * GROUPS : (t + 1) * GROUPS, spot] for t in range(STEPS)], 1
    )
    alive = jnp.concatenate([live[0:1, :]] * STEPS, 1) > 0
    iota = lax.broadcasted_iota(I32, (CLASSES, STEPS * count), 0)
    for g in range(GROUPS):
        own = turned[g * CLASSES : (g + 1) * CLASSES, :]
        total = jnp.log(jnp.sum(jnp.exp(own), 0, keepdims=True))
        hot = jnp.broadcast_to(z[g : g + 1, :], own.shape) == iota
        picked = jnp.sum(jnp.where(hot, own, jnp.zeros_like(own)), 0, keepdims=True)
        logp[g : g + 1, :] = jnp.where(alive, picked - total, jnp.zeros_like(total))
    for copy in outgo:
        copy.wait()


def order_kernel(chips, run, idx, *rest):
    logps, out = rest[:-1], rest[-1]
    slots = out.shape[2]
    part = slots // chips
    order = slot_map(idx[1], chips, run, (slots, slots), 1)
    order = jnp.where(order, 1.0, 0.0).astype(BF16)
    for step in range(STEPS):
        value = jnp.concatenate([p[:, step * part : (step + 1) * part] for p in logps], 1)
        total = jnp.zeros(value.shape, F32)
        for _ in range(3):
            piece = value.astype(BF16)
            total = total + jnp.dot(piece, order, preferred_element_type=F32)
            value = value - piece.astype(F32)
        out[step] = total


def fast_on_device(nx, ny):
    def on_device(
        replay_deter,
        replay_stoch,
        send_rows,
        send_counts,
        actions,
        samples,
        w_stoch,
        w_deter,
        act_table,
        w_prior,
    ):
        peers, cap = send_rows.shape
        slots = peers * cap
        deter = replay_deter.shape[1]
        blocks = w_deter.shape[0]
        width = deter // blocks
        cols = 3 * width
        chips = ny // 2
        part = nx * 2 * cap
        rows = nx * part
        lined = width + LANES
        ix = lax.axis_index("gx").astype(I32)
        iy = lax.axis_index("gy").astype(I32)
        idx = jnp.stack([ix, lax.shift_right_logical(iy, 1), iy & 1])
        ring = [(a, (a + 2) % ny) for a in range(ny)]
        partner = swap_pairs(ny, 1)

        def call(kernel, out_shape, ins, outs, scratch=(), mib=40, flops=0, **kwargs):
            def run(*args):
                return pl.pallas_call(
                    kernel,
                    out_shape=out_shape,
                    in_specs=ins,
                    out_specs=outs,
                    scratch_shapes=scratch,
                    compiler_params=params(mib),
                    cost_estimate=pl.CostEstimate(
                        flops=flops, transcendentals=0, bytes_accessed=2**20
                    ),
                    **kwargs,
                )(*args)

            return run

        srows, drows, prows = w_stoch.shape[0], w_deter.shape[1], w_prior.shape[0]
        wide = w_prior.shape[1] // nx
        shard, quarter = call(
            weights_kernel,
            [
                jax.ShapeDtypeStruct((srows + drows, cols), BF16),
                jax.ShapeDtypeStruct((prows, wide), BF16),
            ],
            [SMEM, HBM, HBM, HBM],
            [VMEM, VMEM],
            [pltpu.SemaphoreType.DMA((3,))],
        )(idx, *(pltpu.with_memory_space_constraint(w, pltpu.HBM) for w in (w_stoch, w_deter, w_prior)))
        stops, quarters = [shard], [quarter]
        for _ in range(1, chips):
            stops.append(lax.ppermute(stops[-1], "gy", ring))
            quarters.append(lax.ppermute(quarters[-1], "gy", ring))
        pieces = []
        for piece in stops:
            pieces += [piece, lax.ppermute(piece, "gy", partner)]
        column = call(
            functools.partial(column_kernel, chips, prows),
            jax.ShapeDtypeStruct((chips * prows, wide), BF16),
            [SMEM] + [VMEM] * chips,
            VMEM,
        )(idx, *quarters)
        priors = []
        for k in range(nx):
            piece = lax.ppermute(column, "gx", swap_pairs(nx, k)) if k else column
            priors += [piece, lax.ppermute(piece, "gy", partner)]

        stoch = jnp.transpose(replay_stoch)
        samp = jnp.transpose(samples, (1, 2, 0)).reshape(-1, slots)
        acts = jnp.transpose(actions)
        *held, known = call(
            functools.partial(pack_kernel, chips, nx, cap),
            [jax.ShapeDtypeStruct((slots // 2, lined), I16)] * (2 * nx)
            + [jax.ShapeDtypeStruct((samp.shape[0] + STEPS, slots), I32)],
            [SMEM] * 3 + [VMEM] * 4,
            [VMEM] * (2 * nx + 1),
            [
                pltpu.VMEM((slots, deter), F32),
                pltpu.VMEM((slots, LANES), F32),
                pltpu.VMEM((slots, replay_deter.shape[0]), F32),
            ],
        )(idx, jnp.transpose(send_rows), send_counts, replay_deter, stoch, samp, acts)
        for k in range(nx):
            for l in range(2):
                if k or l:
                    pairs = [
                        (a * ny + b, (a ^ k) * ny + (b ^ l)) for a in range(nx) for b in range(ny)
                    ]
                    n = k * 2 + l
                    held[n] = lax.ppermute(held[n], ("gx", "gy"), pairs)
        given = [known]
        for k in range(1, nx):
            given.append(lax.ppermute(known, "gx", swap_pairs(nx, k)))
        starts = call(
            functools.partial(fold_kernel, chips, nx * cap),
            [jax.ShapeDtypeStruct((2 * nx, nx * cap, lined), I16)] * chips,
            [VMEM] * (2 * nx),
            [VMEM] * chips,
        )(*held)
        starts = list(starts)
        for m in range(1, chips):
            starts[m] = lax.ppermute(starts[m], "gy", swap_pairs(ny, 2 * m))
        placed = []
        early = 2 * chips - 2
        for first, some in ((0, pieces[:early]), (early, pieces[early:])):
            placed = call(
                functools.partial(place_kernel, chips, (srows, drows), first, len(placed)),
                [
                    jax.ShapeDtypeStruct((ny * srows, cols), BF16),
                    jax.ShapeDtypeStruct((ny * drows, cols), BF16),
                ],
                [SMEM] + [ANY] * len(some) + [VMEM] * len(placed),
                [VMEM] * 2,
                [pltpu.SemaphoreType.DMA((2 * len(some),))],
                input_output_aliases={len(some) + 1 + n: n for n in range(len(placed))},
            )(idx, *some, *placed)
        w_all, wd_all = placed

        parts = []
        for m in range(chips):
            *outs, live = call(
                functools.partial(gru_kernel, rows, cap, nx, m),
                [jax.ShapeDtypeStruct((STEPS, part, width), BF16)] * nx
                + [jax.ShapeDtypeStruct((8, part), F32)],
                [SMEM] + [VMEM] * (4 + nx),
                [VMEM] * (nx + 1),
                [
                    pltpu.VMEM((CLASSES, cols), BF16),
                    pltpu.VMEM((GROUPS * CLASSES + CLASSES, STEPS * rows), BF16),
                    pltpu.VMEM((STEPS * rows, cols), F32),
                    pltpu.VMEM((rows, width), F32),
                    pltpu.VMEM((rows, LANES), F32),
                    pltpu.VMEM((GROUPS * STEPS + 8, rows), I32),
                ],
                flops=2 * STEPS * rows * (GROUPS * CLASSES + width) * cols,
            )(idx, starts[m], act_table, w_all, wd_all, *given)
            got = [outs[0]]
            for k in range(1, nx):
                got.append(lax.ppermute(outs[k], "gx", swap_pairs(nx, k)))
            parts.append((live, got))

        wp_all = call(
            functools.partial(prior_weights_kernel, chips, nx, prows),
            jax.ShapeDtypeStruct((deter, GROUPS * CLASSES), BF16),
            [SMEM] + [VMEM] * (2 * nx),
            VMEM,
        )(idx, *priors)

        shape = (nx, chips, 2 * cap, STEPS, deter)
        states = []
        logps = []
        for m in range(chips):
            live, got = parts[m]
            filled, logp = call(
                functools.partial(prior_kernel, nx, m),
                [
                    jax.ShapeDtypeStruct(shape, BF16),
                    jax.ShapeDtypeStruct((GROUPS, STEPS * part), F32),
                ],
                [SMEM] + [VMEM] * (3 + nx) + [ANY] * len(states),
                [ANY, VMEM],
                [
                    pltpu.VMEM((part, STEPS, deter), BF16),
                    pltpu.SemaphoreType.DMA((nx,)),
                ],
                flops=2 * STEPS * part * deter * GROUPS * CLASSES,
                input_output_aliases={4 + nx: 0} if states else {},
            )(idx, known, live, wp_all, *got, *states)
            states = [filled]
            logps.append(logp)
        logp = call(
            functools.partial(order_kernel, chips, 2 * cap),
            jax.ShapeDtypeStruct((STEPS, GROUPS, slots), F32),
            [SMEM] + [VMEM] * chips,
            VMEM,
        )(idx, *logps)
        return (filled.reshape(slots, STEPS, deter), jnp.transpose(logp, (2, 0, 1)))

    return on_device


def ring_gather(shard, count, index):
    chips = count // 2
    chip, core = index // 2, index % 2
    full = jnp.zeros((count,) + shard.shape, shard.dtype)
    piece = shard
    for hop in range(chips):
        if hop:
            piece = lax.ppermute(piece, "gy", [(a, (a + 2) % count) for a in range(count)])
        other = lax.ppermute(piece, "gy", swap_pairs(count, 1))
        place = lax.rem(chip + chips - hop, chips) * 2
        full = lax.dynamic_update_index_in_dim(full, piece, place + core, 0)
        full = lax.dynamic_update_index_in_dim(full, other, place + 1 - core, 0)
    return full


def one_hot(values, count):
    hot = values[..., None] == jnp.arange(count, dtype=jnp.int32)
    return hot.reshape(values.shape[0], -1).astype(jnp.bfloat16)


def plain_on_device(nx, ny):
    def on_device(
        replay_deter,
        replay_stoch,
        send_rows,
        send_counts,
        actions,
        samples,
        w_stoch,
        w_deter,
        act_table,
        w_prior,
    ):
        peers, cap = send_rows.shape
        slots = peers * cap
        deter = replay_deter.shape[1]
        blocks = w_deter.shape[0]
        assert blocks == nx
        width = deter // blocks
        cols = 3 * width
        ix = lax.axis_index("gx")
        iy = lax.axis_index("gy")

        ws = lax.dynamic_slice_in_dim(w_stoch, ix * cols, cols, 1)
        wd = lax.dynamic_index_in_dim(w_deter, ix, 0, keepdims=False)
        wa = lax.dynamic_slice_in_dim(act_table, ix * cols, cols, 1)
        ws = ring_gather(ws, ny, iy).reshape(-1, cols)
        wd = ring_gather(wd, ny, iy).reshape(-1, cols)

        picks = send_rows.reshape(slots)
        start = replay_deter[picks].astype(jnp.float16).reshape(nx, ny, cap, blocks, width)
        mine = jnp.zeros((nx, ny, nx, cap, width), jnp.float16)
        for k in range(nx):
            part = lax.dynamic_index_in_dim(start, ix ^ k, 3, keepdims=False)
            if k:
                part = lax.ppermute(part, "gx", swap_pairs(nx, k))
            mine = lax.dynamic_update_index_in_dim(mine, part, ix ^ k, 2)
        rows = jnp.zeros((nx, nx, ny, cap, width), jnp.float16)
        for k in range(ny):
            part = lax.dynamic_index_in_dim(mine, iy ^ k, 1, keepdims=False)
            if k:
                part = lax.ppermute(part, "gy", swap_pairs(ny, k))
            rows = lax.dynamic_update_index_in_dim(rows, part, iy ^ k, 2)
        state = rows.reshape(nx * slots, width).astype(jnp.float32)

        first = replay_stoch[picks].reshape(nx, ny, cap * GROUPS)
        note = jnp.concatenate([first, send_counts[0].reshape(nx, ny, 1)], 2)
        note = jnp.transpose(note, (1, 0, 2)).astype(jnp.bfloat16)
        note = jnp.broadcast_to(note[None], (nx,) + note.shape).reshape(peers, nx, -1)
        note = lax.all_to_all(note, ("gx", "gy"), split_axis=0, concat_axis=0, tiled=True)
        note = note.astype(jnp.int32)
        first = jnp.transpose(note[:, :, : cap * GROUPS], (1, 0, 2)).reshape(nx * slots, GROUPS)
        counts = lax.dynamic_index_in_dim(note, ix, 1, keepdims=False)[:, cap * GROUPS]
        live = (jnp.arange(cap, dtype=jnp.int32)[None, :] < counts[:, None]).reshape(slots)

        known = jnp.concatenate([samples[:, : STEPS - 1].reshape(slots, -1), actions], 1)
        given = jnp.zeros((nx,) + known.shape, known.dtype)
        for k in range(nx):
            part = lax.ppermute(known, "gx", swap_pairs(nx, k)) if k else known
            given = lax.dynamic_update_index_in_dim(given, part, ix ^ k, 0)
        given = given.reshape(nx * slots, -1)

        wp = ring_gather(w_prior, ny, iy).reshape(deter, -1)

        log_prob = []
        states = []
        for step in range(STEPS):
            z = first if step == 0 else given[:, GROUPS * (step - 1) : GROUPS * step]
            act = given[:, GROUPS * (STEPS - 1) + step]
            gates = (
                jnp.dot(one_hot(z, CLASSES), ws, preferred_element_type=jnp.float32)
                + jnp.dot(
                    one_hot(act, act_table.shape[0]), wa, preferred_element_type=jnp.float32
                )
                + jnp.dot(state.astype(jnp.bfloat16), wd, preferred_element_type=jnp.float32)
            )
            reset = jax.nn.sigmoid(gates[:, :width])
            cand = jnp.tanh(reset * gates[:, width : 2 * width])
            update = jax.nn.sigmoid(gates[:, 2 * width :] - 1.0)
            state = update * cand + (1.0 - update) * state
            out = state.astype(jnp.bfloat16).reshape(nx, slots, width)
            whole = jnp.zeros((slots, deter), jnp.bfloat16)
            for k in range(nx):
                part = lax.dynamic_index_in_dim(out, ix ^ k, 0, keepdims=False)
                if k:
                    part = lax.ppermute(part, "gx", swap_pairs(nx, k))
                whole = lax.dynamic_update_slice_in_dim(whole, part, (ix ^ k) * width, 1)
            whole = jnp.where(live[:, None], whole, jnp.zeros_like(whole))
            states.append(whole)
            logits = jnp.dot(whole, wp, preferred_element_type=jnp.float32)
            logits = logits.reshape(slots, GROUPS, CLASSES)
            totals = jnp.log(jnp.sum(jnp.exp(logits), -1))
            hits = samples[:, step, :, None] == jnp.arange(CLASSES, dtype=jnp.int32)
            picked = jnp.sum(jnp.where(hits, logits, jnp.zeros_like(logits)), -1)
            log_prob.append(jnp.where(live[:, None], picked - totals, jnp.zeros_like(totals)))
        return (jnp.stack(states, 1), jnp.stack(log_prob, 1))

    return on_device


def solution(mesh):
    nx, ny = mesh.shape["gx"], mesh.shape["gy"]

    def on_device(*args):
        if args[2].shape[1] % 8 == 0 and ny == 8:
            return fast_on_device(nx, ny)(*args)
        return plain_on_device(nx, ny)(*args)

    in_specs = (
        P(("gx", "gy"), None),
        P(("gx", "gy"), None),
        P(("gx", "gy"), None),
        P(("gx", "gy"), None),
        P(("gx", "gy"), None),
        P(("gx", "gy"), None, None),
        P("gy", None),
        P(None, "gy", None),
        P(),
        P("gy", None),
    )
    out_specs = (P(("gx", "gy"), None, None), P(("gx", "gy"), None, None))
    return jax.shard_map(
        on_device, mesh=mesh, in_specs=in_specs, out_specs=out_specs, check_vma=False
    )
```

```python
import functools
import jax
import jax.numpy as jnp
from jax import lax
from jax.experimental import pallas as pl
from jax.experimental.pallas import tpu as pltpu
from jax.sharding import PartitionSpec as P


GROUPS = 32
CLASSES = 32
STEPS = 4
LANES = 128
SCALE = 32767.0
BF16 = jnp.bfloat16
F32 = jnp.float32
I32 = jnp.int32
I16 = jnp.int16


VMEM = pl.BlockSpec(memory_space=pltpu.VMEM)
SMEM = pl.BlockSpec(memory_space=pltpu.SMEM)
ANY = pl.BlockSpec(memory_space=pl.ANY)
HBM = pl.BlockSpec(memory_space=pltpu.HBM)


def params(mib):
    return pltpu.CompilerParams(vmem_limit_bytes=mib * 2**20)


def swap_pairs(count, mask):
    return [(a, a ^ mask) for a in range(count)]


def shard_of(chip, core, chips, n):
    return lax.rem(chip + chips - n // 2, chips) * 2 + (core ^ (n % 2))


def weights_kernel(idx, w_stoch, w_deter, w_prior, stoch, deter, quarter, sems):
    cols, wide = stoch.shape[1], quarter.shape[1]
    at = pl.multiple_of(idx[0] * cols, cols)
    copies = [
        pltpu.make_async_copy(w_stoch.at[:, pl.ds(at, cols)], stoch, sems.at[0]),
        pltpu.make_async_copy(w_deter.at[idx[0]], deter, sems.at[1]),
        pltpu.make_async_copy(
            w_prior.at[:, pl.ds(pl.multiple_of(idx[0] * wide, wide), wide)], quarter, sems.at[2]
        ),
    ]
    for copy in copies:
        copy.start()
    for copy in copies:
        copy.wait()


def slot_map(chip, chips, run, shape, slot_dim):
    slot = lax.broadcasted_iota(I32, shape, slot_dim)
    place = lax.broadcasted_iota(I32, shape, 1 - slot_dim)
    part = shape[0] // chips
    chunk, rest = place // part, place % part
    return slot == ((rest // run) * chips + (chunk ^ chip)) * run + rest % run


def pack_kernel(chips, nx, cap, idx, rows_ref, counts, deter, stoch, samples, acts, *rest):
    outs = rest[: 2 * nx]
    known = rest[2 * nx]
    s_s, f_s, p_s = rest[2 * nx + 1 :]
    ix, chip, core = idx[0], idx[1], idx[2]
    slots = s_s.shape[0]
    half = slots // 2
    width = outs[0].shape[1] - LANES
    lane = lax.broadcasted_iota(I32, (1, LANES), 1)
    spot = lax.broadcasted_iota(I32, (1, deter.shape[0]), 1)

    def one_dest(n, carry):
        l = n // (chips * nx)
        m = (n // nx) % chips
        o = n % nx
        dest = (o * chips + (m ^ chip)) * 2 + (l ^ core)
        count = counts[0, dest]
        for c in range(cap):
            src = rows_ref[c, dest]
            s_s[pl.ds(n * cap + c, 1), :] = deter[pl.ds(src, 1), :]
            p_s[pl.ds(n * cap + c, 1), :] = jnp.where(spot == src, 1.0, 0.0)
            f_s[pl.ds(n * cap + c, 1), :] = jnp.where(
                lane == GROUPS, jnp.where(count > c, 1.0, 0.0), 0.0
            )
        return carry

    lax.fori_loop(0, slots // cap, one_dest, 0)
    f_s[:, 0 : stoch.shape[0]] = lax.dot_general(
        p_s[...].astype(BF16),
        stoch[...].astype(F32).astype(BF16),
        (((1,), (1,)), ((), ())),
        preferred_element_type=F32,
    )
    for k in range(nx):
        at = pl.multiple_of((ix ^ k) * width, width)
        for l in range(2):
            part = s_s[l * half : (l + 1) * half, pl.ds(at, width)]
            out = outs[k * 2 + l]
            out[:, :width] = jnp.round(part * SCALE).astype(I32).astype(I16)
            out[:, width:] = f_s[l * half : (l + 1) * half, :].astype(I32).astype(I16)
    order = slot_map(chip, chips, 2 * cap, (slots, slots), 0)
    order = jnp.where(order, 1.0, 0.0).astype(BF16)
    tail = samples.shape[0]
    known[tail + STEPS :, :] = jnp.zeros((known.shape[0] - tail - STEPS, slots), I16)
    known[0:tail, :] = jnp.dot(
        samples[...].astype(F32).astype(BF16), order, preferred_element_type=F32
    ).astype(I32).astype(I16)
    known[tail : tail + STEPS, :] = jnp.dot(
        acts[...].astype(F32).astype(BF16), order, preferred_element_type=F32
    ).astype(I32).astype(I16)


def fold_kernel(chips, run, *rest):
    pieces, outs = rest[:-chips], rest[-chips:]
    for m in range(chips):
        for n, piece in enumerate(pieces):
            outs[m][n] = piece[m * run : (m + 1) * run, :]


def place_kernel(chips, runs, first, held, idx, *rest):
    count = len(runs)
    outs = rest[-count:]
    pieces = rest[: len(rest) - count - held]
    each = len(pieces) // count
    for o, run in enumerate(runs):
        for n in range(each):
            place = shard_of(idx[1], idx[2], chips, n + first) * run
            outs[o][pl.ds(pl.multiple_of(place, run), run), :] = pieces[o * each + n][...]


def column_kernel(chips, run, idx, *rest):
    pieces, out = rest[:-1], rest[-1]
    for hop, piece in enumerate(pieces):
        place = lax.rem(idx[1] + chips - hop, chips) * run
        out[pl.ds(pl.multiple_of(place, run), run), :] = piece[...]


def prior_weights_kernel(chips, nx, run, idx, *rest):
    pieces, out = rest[:-1], rest[-1]
    wide = out.shape[1] // nx
    for n, piece in enumerate(pieces):
        at = pl.multiple_of((idx[0] ^ (n // 2)) * wide, wide)
        for z in range(chips):
            place = (z * 2 + (idx[2] ^ (n % 2))) * run
            out[pl.ds(pl.multiple_of(place, run), run), pl.ds(at, wide)] = piece[
                z * run : (z + 1) * run, :
            ]


def gru_kernel(rows, cap, nx, m, idx, x, act_table, w_s, wd_s, *rest):
    given = rest[:nx]
    outs = rest[nx : 2 * nx]
    live, wa_s, oh_s, g_s, h_s, f_s, z_s = rest[2 * nx :]
    ix, core = idx[0], idx[2]
    width = wd_s.shape[0]
    kinds = w_s.shape[0]
    cols = w_s.shape[1]
    part = rows // nx
    wa_s[...] = jnp.zeros(wa_s.shape, BF16)
    wa_s[0 : act_table.shape[0], :] = act_table[:, pl.ds(pl.multiple_of(ix * cols, cols), cols)]
    for k in range(nx):
        for l in range(2):
            got = x[k * 2 + l].astype(I32).astype(F32)
            for o in range(nx):
                place = (ix ^ o) * part + (ix ^ k) * (2 * cap) + (core ^ l) * cap
                at = pl.ds(pl.multiple_of(place, cap), cap)
                h_s[at, :] = got[o * cap : (o + 1) * cap, :width] * (1.0 / SCALE)
                f_s[at, :] = got[o * cap : (o + 1) * cap, width:]
    turned = f_s[...].T
    live[...] = turned[GROUPS : GROUPS + 8, 0:part]
    tail = GROUPS * STEPS
    z_s[0:GROUPS, :] = turned[0:GROUPS, :].astype(I32)
    spot = slice(m * part, (m + 1) * part)
    z_s[GROUPS : GROUPS * STEPS, :] = jnp.concatenate(
        [g[0 : GROUPS * (STEPS - 1), spot].astype(I32) for g in given], 1
    )
    z_s[tail : tail + STEPS, :] = jnp.concatenate(
        [g[tail : tail + 16, spot].astype(I32)[:STEPS] for g in given], 1
    )
    iota = lax.broadcasted_iota(I32, (CLASSES, rows), 0)
    for step in range(STEPS):
        for g in range(GROUPS + 1):
            row = step * GROUPS + g if g < GROUPS else tail + step
            hot = jnp.broadcast_to(z_s[row : row + 1, :], (CLASSES, rows)) == iota
            oh_s[g * CLASSES : (g + 1) * CLASSES, step * rows : (step + 1) * rows] = jnp.where(
                hot, 1.0, 0.0
            ).astype(BF16)
    dims = (((0,), (0,)), ((), ()))
    g_s[...] = lax.dot_general(
        oh_s[0:kinds, :], w_s[...], dims, preferred_element_type=F32
    ) + lax.dot_general(oh_s[kinds:, :], wa_s[...], dims, preferred_element_type=F32)
    keep = jnp.broadcast_to(f_s[:, GROUPS : GROUPS + 1], (rows, width)) > 0
    for step in range(STEPS):
        h = h_s[...]
        gates = g_s[step * rows : (step + 1) * rows, :] + jnp.dot(
            h.astype(BF16), wd_s[...], preferred_element_type=F32
        )
        reset = jax.nn.sigmoid(gates[:, :width])
        cand = jnp.tanh(reset * gates[:, width : 2 * width])
        update = jax.nn.sigmoid(gates[:, 2 * width :] - 1.0)
        h = update * cand + (1.0 - update) * h
        h_s[...] = h
        shown = jnp.where(keep, h, jnp.zeros_like(h)).astype(BF16)
        for k in range(nx):
            outs[k][step] = shown[k * part : (k + 1) * part, :]


def prior_kernel(nx, m, idx, known, live, wp_s, *rest):
    parts = rest[:nx]
    states, logp, st_s, out_sems = rest[-4:]
    ix, chip = idx[0], idx[1]
    width = parts[0].shape[2]
    count = parts[0].shape[1]
    for k in range(nx):
        at = pl.multiple_of((ix ^ k) * width, width)
        st_s[:, :, pl.ds(at, width)] = jnp.transpose(parts[k][...], (1, 0, 2))
    outgo = []
    run = count // nx
    for a in range(nx):
        outgo.append(
            pltpu.make_async_copy(
                st_s.at[pl.ds(a * run, run)], states.at[a, chip ^ m], out_sems.at[a]
            )
        )
    for copy in outgo:
        copy.start()
    logits = jnp.zeros((STEPS * count, wp_s.shape[1]), F32)
    for k in range(nx):
        at = pl.multiple_of((ix ^ k) * width, width)
        part = parts[k][...].reshape(STEPS * count, width)
        logits = logits + jnp.dot(part, wp_s[pl.ds(at, width), :], preferred_element_type=F32)
    turned = logits.T
    spot = slice(m * count, (m + 1) * count)
    z = jnp.concatenate(
        [known[t * GROUPS : (t + 1) * GROUPS, spot].astype(I32) for t in range(STEPS)], 1
    )
    alive = jnp.concatenate([live[0:1, :]] * STEPS, 1) > 0
    iota = lax.broadcasted_iota(I32, (CLASSES, STEPS * count), 0)
    for g in range(GROUPS):
        own = turned[g * CLASSES : (g + 1) * CLASSES, :]
        total = jnp.log(jnp.sum(jnp.exp(own), 0, keepdims=True))
        hot = jnp.broadcast_to(z[g : g + 1, :], own.shape) == iota
        picked = jnp.sum(jnp.where(hot, own, jnp.zeros_like(own)), 0, keepdims=True)
        logp[g : g + 1, :] = jnp.where(alive, picked - total, jnp.zeros_like(total))
    for copy in outgo:
        copy.wait()


def order_kernel(chips, run, idx, *rest):
    logps, out = rest[:-1], rest[-1]
    slots = out.shape[2]
    part = slots // chips
    order = slot_map(idx[1], chips, run, (slots, slots), 1)
    order = jnp.where(order, 1.0, 0.0).astype(BF16)
    for step in range(STEPS):
        value = jnp.concatenate([p[:, step * part : (step + 1) * part] for p in logps], 1)
        total = jnp.zeros(value.shape, F32)
        for _ in range(3):
            piece = value.astype(BF16)
            total = total + jnp.dot(piece, order, preferred_element_type=F32)
            value = value - piece.astype(F32)
        out[step] = total


def fast_on_device(nx, ny):
    def on_device(
        replay_deter,
        replay_stoch,
        send_rows,
        send_counts,
        actions,
        samples,
        w_stoch,
        w_deter,
        act_table,
        w_prior,
    ):
        peers, cap = send_rows.shape
        slots = peers * cap
        deter = replay_deter.shape[1]
        blocks = w_deter.shape[0]
        width = deter // blocks
        cols = 3 * width
        chips = ny // 2
        part = nx * 2 * cap
        rows = nx * part
        lined = width + LANES
        ix = lax.axis_index("gx").astype(I32)
        iy = lax.axis_index("gy").astype(I32)
        idx = jnp.stack([ix, lax.shift_right_logical(iy, 1), iy & 1])
        ring = [(a, (a + 2) % ny) for a in range(ny)]
        partner = swap_pairs(ny, 1)

        def call(kernel, out_shape, ins, outs, scratch=(), mib=16, flops=0, **kwargs):
            def run(*args):
                return pl.pallas_call(
                    kernel,
                    out_shape=out_shape,
                    in_specs=ins,
                    out_specs=outs,
                    scratch_shapes=scratch,
                    compiler_params=params(mib),
                    cost_estimate=pl.CostEstimate(
                        flops=flops, transcendentals=0, bytes_accessed=2**20
                    ),
                    **kwargs,
                )(*args)

            return run

        srows, drows, prows = w_stoch.shape[0], w_deter.shape[1], w_prior.shape[0]
        wide = w_prior.shape[1] // nx
        own = call(
            weights_kernel,
            [
                jax.ShapeDtypeStruct((srows, cols), BF16),
                jax.ShapeDtypeStruct((drows, cols), BF16),
                jax.ShapeDtypeStruct((prows, wide), BF16),
            ],
            [SMEM, HBM, HBM, HBM],
            [VMEM] * 3,
            [pltpu.SemaphoreType.DMA((3,))],
        )(idx, *(pltpu.with_memory_space_constraint(w, pltpu.HBM) for w in (w_stoch, w_deter, w_prior)))
        stops = {}
        for name, shard in zip("sdp", own):
            stops[name] = [shard]
            for _ in range(1, chips):
                stops[name].append(lax.ppermute(stops[name][-1], "gy", ring))
        pieces = {}
        for name in "sd":
            pieces[name] = []
            for piece in stops[name]:
                pieces[name] += [piece, lax.ppermute(piece, "gy", partner)]
        column = call(
            functools.partial(column_kernel, chips, prows),
            jax.ShapeDtypeStruct((chips * prows, wide), BF16),
            [SMEM] + [VMEM] * chips,
            VMEM,
        )(idx, *stops["p"])
        priors = []
        for k in range(nx):
            piece = lax.ppermute(column, "gx", swap_pairs(nx, k)) if k else column
            priors += [piece, lax.ppermute(piece, "gy", partner)]

        stoch = jnp.transpose(replay_stoch)
        samp = jnp.transpose(samples, (1, 2, 0)).reshape(-1, slots)
        acts = jnp.transpose(actions)
        *held, known = call(
            functools.partial(pack_kernel, chips, nx, cap),
            [jax.ShapeDtypeStruct((slots // 2, lined), I16)] * (2 * nx)
            + [jax.ShapeDtypeStruct((samp.shape[0] + 16, slots), I16)],
            [SMEM] * 3 + [VMEM] * 4,
            [VMEM] * (2 * nx + 1),
            [
                pltpu.VMEM((slots, deter), F32),
                pltpu.VMEM((slots, LANES), F32),
                pltpu.VMEM((slots, replay_deter.shape[0]), F32),
            ],
        )(idx, jnp.transpose(send_rows), send_counts, replay_deter, stoch, samp, acts)
        for k in range(nx):
            for l in range(2):
                if k or l:
                    pairs = [
                        (a * ny + b, (a ^ k) * ny + (b ^ l)) for a in range(nx) for b in range(ny)
                    ]
                    n = k * 2 + l
                    held[n] = lax.ppermute(held[n], ("gx", "gy"), pairs)
        given = [known]
        for k in range(1, nx):
            given.append(lax.ppermute(known, "gx", swap_pairs(nx, k)))
        starts = call(
            functools.partial(fold_kernel, chips, nx * cap),
            [jax.ShapeDtypeStruct((2 * nx, nx * cap, lined), I16)] * chips,
            [VMEM] * (2 * nx),
            [VMEM] * chips,
        )(*held)
        starts = list(starts)
        for m in range(1, chips):
            starts[m] = lax.ppermute(starts[m], "gy", swap_pairs(ny, 2 * m))
        placed = []
        early = 2 * chips - 2
        for first, end in ((0, early), (early, 2 * chips)):
            some = pieces["s"][first:end] + pieces["d"][first:end]
            placed = call(
                functools.partial(place_kernel, chips, (srows, drows), first, len(placed)),
                [
                    jax.ShapeDtypeStruct((ny * srows, cols), BF16),
                    jax.ShapeDtypeStruct((ny * drows, cols), BF16),
                ],
                [SMEM] + [VMEM] * (len(some) + len(placed)),
                [VMEM] * 2,
                input_output_aliases={len(some) + 1 + n: n for n in range(len(placed))},
            )(idx, *some, *placed)
        w_all, wd_all = placed

        parts = []
        for m in range(chips):
            *outs, live = call(
                functools.partial(gru_kernel, rows, cap, nx, m),
                [jax.ShapeDtypeStruct((STEPS, part, width), BF16)] * nx
                + [jax.ShapeDtypeStruct((8, part), F32)],
                [SMEM] + [VMEM] * (4 + nx),
                [VMEM] * (nx + 1),
                [
                    pltpu.VMEM((CLASSES, cols), BF16),
                    pltpu.VMEM((GROUPS * CLASSES + CLASSES, STEPS * rows), BF16),
                    pltpu.VMEM((STEPS * rows, cols), F32),
                    pltpu.VMEM((rows, width), F32),
                    pltpu.VMEM((rows, LANES), F32),
                    pltpu.VMEM((GROUPS * STEPS + 8, rows), I32),
                ],
                flops=2 * STEPS * rows * (GROUPS * CLASSES + width) * cols,
            )(idx, starts[m], act_table, w_all, wd_all, *given)
            got = [outs[0]]
            for k in range(1, nx):
                got.append(lax.ppermute(outs[k], "gx", swap_pairs(nx, k)))
            parts.append((live, got))

        wp_all = call(
            functools.partial(prior_weights_kernel, chips, nx, prows),
            jax.ShapeDtypeStruct((deter, GROUPS * CLASSES), BF16),
            [SMEM] + [VMEM] * (2 * nx),
            VMEM,
        )(idx, *priors)

        shape = (nx, chips, 2 * cap, STEPS, deter)
        states = []
        logps = []
        for m in range(chips):
            live, got = parts[m]
            filled, logp = call(
                functools.partial(prior_kernel, nx, m),
                [
                    jax.ShapeDtypeStruct(shape, BF16),
                    jax.ShapeDtypeStruct((GROUPS, STEPS * part), F32),
                ],
                [SMEM] + [VMEM] * (3 + nx) + [ANY] * len(states),
                [ANY, VMEM],
                [
                    pltpu.VMEM((part, STEPS, deter), BF16),
                    pltpu.SemaphoreType.DMA((nx,)),
                ],
                flops=2 * STEPS * part * deter * GROUPS * CLASSES,
                input_output_aliases={4 + nx: 0} if states else {},
            )(idx, known, live, wp_all, *got, *states)
            states = [filled]
            logps.append(logp)
        logp = call(
            functools.partial(order_kernel, chips, 2 * cap),
            jax.ShapeDtypeStruct((STEPS, GROUPS, slots), F32),
            [SMEM] + [VMEM] * chips,
            VMEM,
        )(idx, *logps)
        return (filled.reshape(slots, STEPS, deter), jnp.transpose(logp, (2, 0, 1)))

    return on_device


def ring_gather(shard, count, index):
    chips = count // 2
    chip, core = index // 2, index % 2
    full = jnp.zeros((count,) + shard.shape, shard.dtype)
    piece = shard
    for hop in range(chips):
        if hop:
            piece = lax.ppermute(piece, "gy", [(a, (a + 2) % count) for a in range(count)])
        other = lax.ppermute(piece, "gy", swap_pairs(count, 1))
        place = lax.rem(chip + chips - hop, chips) * 2
        full = lax.dynamic_update_index_in_dim(full, piece, place + core, 0)
        full = lax.dynamic_update_index_in_dim(full, other, place + 1 - core, 0)
    return full


def one_hot(values, count):
    hot = values[..., None] == jnp.arange(count, dtype=jnp.int32)
    return hot.reshape(values.shape[0], -1).astype(jnp.bfloat16)


def plain_on_device(nx, ny):
    def on_device(
        replay_deter,
        replay_stoch,
        send_rows,
        send_counts,
        actions,
        samples,
        w_stoch,
        w_deter,
        act_table,
        w_prior,
    ):
        peers, cap = send_rows.shape
        slots = peers * cap
        deter = replay_deter.shape[1]
        blocks = w_deter.shape[0]
        assert blocks == nx
        width = deter // blocks
        cols = 3 * width
        ix = lax.axis_index("gx")
        iy = lax.axis_index("gy")

        ws = lax.dynamic_slice_in_dim(w_stoch, ix * cols, cols, 1)
        wd = lax.dynamic_index_in_dim(w_deter, ix, 0, keepdims=False)
        wa = lax.dynamic_slice_in_dim(act_table, ix * cols, cols, 1)
        ws = ring_gather(ws, ny, iy).reshape(-1, cols)
        wd = ring_gather(wd, ny, iy).reshape(-1, cols)

        picks = send_rows.reshape(slots)
        start = replay_deter[picks].astype(jnp.float16).reshape(nx, ny, cap, blocks, width)
        mine = jnp.zeros((nx, ny, nx, cap, width), jnp.float16)
        for k in range(nx):
            part = lax.dynamic_index_in_dim(start, ix ^ k, 3, keepdims=False)
            if k:
                part = lax.ppermute(part, "gx", swap_pairs(nx, k))
            mine = lax.dynamic_update_index_in_dim(mine, part, ix ^ k, 2)
        rows = jnp.zeros((nx, nx, ny, cap, width), jnp.float16)
        for k in range(ny):
            part = lax.dynamic_index_in_dim(mine, iy ^ k, 1, keepdims=False)
            if k:
                part = lax.ppermute(part, "gy", swap_pairs(ny, k))
            rows = lax.dynamic_update_index_in_dim(rows, part, iy ^ k, 2)
        state = rows.reshape(nx * slots, width).astype(jnp.float32)

        first = replay_stoch[picks].reshape(nx, ny, cap * GROUPS)
        note = jnp.concatenate([first, send_counts[0].reshape(nx, ny, 1)], 2)
        note = jnp.transpose(note, (1, 0, 2)).astype(jnp.bfloat16)
        note = jnp.broadcast_to(note[None], (nx,) + note.shape).reshape(peers, nx, -1)
        note = lax.all_to_all(note, ("gx", "gy"), split_axis=0, concat_axis=0, tiled=True)
        note = note.astype(jnp.int32)
        first = jnp.transpose(note[:, :, : cap * GROUPS], (1, 0, 2)).reshape(nx * slots, GROUPS)
        counts = lax.dynamic_index_in_dim(note, ix, 1, keepdims=False)[:, cap * GROUPS]
        live = (jnp.arange(cap, dtype=jnp.int32)[None, :] < counts[:, None]).reshape(slots)

        known = jnp.concatenate([samples[:, : STEPS - 1].reshape(slots, -1), actions], 1)
        given = jnp.zeros((nx,) + known.shape, known.dtype)
        for k in range(nx):
            part = lax.ppermute(known, "gx", swap_pairs(nx, k)) if k else known
            given = lax.dynamic_update_index_in_dim(given, part, ix ^ k, 0)
        given = given.reshape(nx * slots, -1)

        wp = ring_gather(w_prior, ny, iy).reshape(deter, -1)

        log_prob = []
        states = []
        for step in range(STEPS):
            z = first if step == 0 else given[:, GROUPS * (step - 1) : GROUPS * step]
            act = given[:, GROUPS * (STEPS - 1) + step]
            gates = (
                jnp.dot(one_hot(z, CLASSES), ws, preferred_element_type=jnp.float32)
                + jnp.dot(
                    one_hot(act, act_table.shape[0]), wa, preferred_element_type=jnp.float32
                )
                + jnp.dot(state.astype(jnp.bfloat16), wd, preferred_element_type=jnp.float32)
            )
            reset = jax.nn.sigmoid(gates[:, :width])
            cand = jnp.tanh(reset * gates[:, width : 2 * width])
            update = jax.nn.sigmoid(gates[:, 2 * width :] - 1.0)
            state = update * cand + (1.0 - update) * state
            out = state.astype(jnp.bfloat16).reshape(nx, slots, width)
            whole = jnp.zeros((slots, deter), jnp.bfloat16)
            for k in range(nx):
                part = lax.dynamic_index_in_dim(out, ix ^ k, 0, keepdims=False)
                if k:
                    part = lax.ppermute(part, "gx", swap_pairs(nx, k))
                whole = lax.dynamic_update_slice_in_dim(whole, part, (ix ^ k) * width, 1)
            whole = jnp.where(live[:, None], whole, jnp.zeros_like(whole))
            states.append(whole)
            logits = jnp.dot(whole, wp, preferred_element_type=jnp.float32)
            logits = logits.reshape(slots, GROUPS, CLASSES)
            totals = jnp.log(jnp.sum(jnp.exp(logits), -1))
            hits = samples[:, step, :, None] == jnp.arange(CLASSES, dtype=jnp.int32)
            picked = jnp.sum(jnp.where(hits, logits, jnp.zeros_like(logits)), -1)
            log_prob.append(jnp.where(live[:, None], picked - totals, jnp.zeros_like(totals)))
        return (jnp.stack(states, 1), jnp.stack(log_prob, 1))

    return on_device


def solution(mesh):
    nx, ny = mesh.shape["gx"], mesh.shape["gy"]

    def on_device(*args):
        if args[2].shape[1] % 8 == 0 and ny == 8:
            return fast_on_device(nx, ny)(*args)
        return plain_on_device(nx, ny)(*args)

    in_specs = (
        P(("gx", "gy"), None),
        P(("gx", "gy"), None),
        P(("gx", "gy"), None),
        P(("gx", "gy"), None),
        P(("gx", "gy"), None),
        P(("gx", "gy"), None, None),
        P("gy", None),
        P(None, "gy", None),
        P(),
        P("gy", None),
    )
    out_specs = (P(("gx", "gy"), None, None), P(("gx", "gy"), None, None))
    return jax.shard_map(
        on_device, mesh=mesh, in_specs=in_specs, out_specs=out_specs, check_vma=False
    )
```

```python
import functools
import jax
import jax.numpy as jnp
from jax import lax
from jax.experimental import pallas as pl
from jax.experimental.pallas import tpu as pltpu
from jax.sharding import PartitionSpec as P


GROUPS = 32
CLASSES = 32
STEPS = 4
LANES = 128
SCALE = 32767.0
BF16 = jnp.bfloat16
F32 = jnp.float32
I32 = jnp.int32
I16 = jnp.int16


VMEM = pl.BlockSpec(memory_space=pltpu.VMEM)
SMEM = pl.BlockSpec(memory_space=pltpu.SMEM)
ANY = pl.BlockSpec(memory_space=pl.ANY)
HBM = pl.BlockSpec(memory_space=pltpu.HBM)


def params(mib):
    return pltpu.CompilerParams(vmem_limit_bytes=mib * 2**20)


def swap_pairs(count, mask):
    return [(a, a ^ mask) for a in range(count)]


def shard_of(chip, core, chips, n):
    return lax.rem(chip + chips - n // 2, chips) * 2 + (core ^ (n % 2))


def weights_kernel(idx, w_stoch, w_deter, w_prior, stoch, deter, quarter, sems):
    cols, wide = stoch.shape[1], quarter.shape[1]
    at = pl.multiple_of(idx[0] * cols, cols)
    copies = [
        pltpu.make_async_copy(w_stoch.at[:, pl.ds(at, cols)], stoch, sems.at[0]),
        pltpu.make_async_copy(w_deter.at[idx[0]], deter, sems.at[1]),
        pltpu.make_async_copy(
            w_prior.at[:, pl.ds(pl.multiple_of(idx[0] * wide, wide), wide)], quarter, sems.at[2]
        ),
    ]
    for copy in copies:
        copy.start()
    for copy in copies:
        copy.wait()


def slot_map(chip, chips, run, shape, slot_dim):
    slot = lax.broadcasted_iota(I32, shape, slot_dim)
    place = lax.broadcasted_iota(I32, shape, 1 - slot_dim)
    part = shape[0] // chips
    chunk, rest = place // part, place % part
    return slot == ((rest // run) * chips + (chunk ^ chip)) * run + rest % run


def pack_kernel(chips, nx, cap, idx, rows_ref, counts, deter, stoch, samples, acts, *rest):
    outs = rest[: 2 * nx]
    known = rest[2 * nx]
    s_s, f_s, p_s = rest[2 * nx + 1 :]
    ix, chip, core = idx[0], idx[1], idx[2]
    slots = s_s.shape[0]
    half = slots // 2
    width = outs[0].shape[1] - LANES
    lane = lax.broadcasted_iota(I32, (1, LANES), 1)
    spot = lax.broadcasted_iota(I32, (1, deter.shape[0]), 1)

    def one_dest(n, carry):
        l = n // (chips * nx)
        m = (n // nx) % chips
        o = n % nx
        dest = (o * chips + (m ^ chip)) * 2 + (l ^ core)
        count = counts[0, dest]
        for c in range(cap):
            src = rows_ref[c, dest]
            s_s[pl.ds(n * cap + c, 1), :] = deter[pl.ds(src, 1), :]
            p_s[pl.ds(n * cap + c, 1), :] = jnp.where(spot == src, 1.0, 0.0)
            f_s[pl.ds(n * cap + c, 1), :] = jnp.where(
                lane == GROUPS, jnp.where(count > c, 1.0, 0.0), 0.0
            )
        return carry

    lax.fori_loop(0, slots // cap, one_dest, 0)
    f_s[:, 0 : stoch.shape[0]] = lax.dot_general(
        p_s[...].astype(BF16),
        stoch[...].astype(F32).astype(BF16),
        (((1,), (1,)), ((), ())),
        preferred_element_type=F32,
    )
    for k in range(nx):
        at = pl.multiple_of((ix ^ k) * width, width)
        for l in range(2):
            part = s_s[l * half : (l + 1) * half, pl.ds(at, width)]
            out = outs[k * 2 + l]
            out[:, :width] = jnp.round(part * SCALE).astype(I32).astype(I16)
            out[:, width:] = f_s[l * half : (l + 1) * half, :].astype(I32).astype(I16)
    order = slot_map(chip, chips, 2 * cap, (slots, slots), 0)
    order = jnp.where(order, 1.0, 0.0).astype(BF16)
    tail = samples.shape[0]
    known[tail + STEPS :, :] = jnp.zeros((known.shape[0] - tail - STEPS, slots), I16)
    known[0:tail, :] = jnp.dot(
        samples[...].astype(F32).astype(BF16), order, preferred_element_type=F32
    ).astype(I32).astype(I16)
    known[tail : tail + STEPS, :] = jnp.dot(
        acts[...].astype(F32).astype(BF16), order, preferred_element_type=F32
    ).astype(I32).astype(I16)


def fold_kernel(chips, run, *rest):
    pieces, outs = rest[:-chips], rest[-chips:]
    for m in range(chips):
        for n, piece in enumerate(pieces):
            outs[m][n] = piece[m * run : (m + 1) * run, :]


def place_kernel(chips, runs, first, held, idx, *rest):
    count = len(runs)
    outs = rest[-count:]
    pieces = rest[: len(rest) - count - held]
    each = len(pieces) // count
    for o, run in enumerate(runs):
        for n in range(each):
            place = shard_of(idx[1], idx[2], chips, n + first) * run
            outs[o][pl.ds(pl.multiple_of(place, run), run), :] = pieces[o * each + n][...]


def column_kernel(chips, run, idx, *rest):
    pieces, out = rest[:-1], rest[-1]
    for hop, piece in enumerate(pieces):
        place = lax.rem(idx[1] + chips - hop, chips) * run
        out[pl.ds(pl.multiple_of(place, run), run), :] = piece[...]


def prior_weights_kernel(chips, nx, run, idx, *rest):
    pieces, out = rest[:-1], rest[-1]
    wide = out.shape[1] // nx
    for n, piece in enumerate(pieces):
        at = pl.multiple_of((idx[0] ^ (n // 2)) * wide, wide)
        for z in range(chips):
            place = (z * 2 + (idx[2] ^ (n % 2))) * run
            out[pl.ds(pl.multiple_of(place, run), run), pl.ds(at, wide)] = piece[
                z * run : (z + 1) * run, :
            ]


def acts_kernel(chips, rows, nx, idx, act_table, *rest):
    given, (out, wa_s, z_s, oh_s) = rest[:nx], rest[nx:]
    cols = wa_s.shape[1]
    part = rows // nx
    tail = GROUPS * STEPS
    wa_s[...] = jnp.zeros(wa_s.shape, BF16)
    wa_s[0 : act_table.shape[0], :] = act_table[
        :, pl.ds(pl.multiple_of(idx[0] * cols, cols), cols)
    ]
    for m in range(chips):
        spot = slice(m * part, (m + 1) * part)
        z_s[m] = jnp.concatenate([g[tail : tail + 16, spot].astype(I32)[:8] for g in given], 1)
    iota = lax.broadcasted_iota(I32, (CLASSES, rows), 0)

    def one_chunk(m, carry):
        z = z_s[m]
        for step in range(STEPS):
            hot = jnp.broadcast_to(z[step : step + 1, :], (CLASSES, rows)) == iota
            oh_s[:, step * rows : (step + 1) * rows] = jnp.where(hot, 1.0, 0.0).astype(BF16)
        out[m] = lax.dot_general(
            oh_s[...], wa_s[...], (((0,), (0,)), ((), ())), preferred_element_type=F32
        ).astype(BF16)
        return carry

    lax.fori_loop(0, chips, one_chunk, 0)


def gru_kernel(rows, cap, nx, m, idx, x, acts, w_s, wd_s, *rest):
    given = rest[:nx]
    outs = rest[nx : 2 * nx]
    live, oh_s, g_s, h_s, f_s, z_s = rest[2 * nx :]
    ix, core = idx[0], idx[2]
    width = wd_s.shape[0]
    part = rows // nx
    for k in range(nx):
        for l in range(2):
            got = x[k * 2 + l].astype(I32).astype(F32)
            for o in range(nx):
                place = (ix ^ o) * part + (ix ^ k) * (2 * cap) + (core ^ l) * cap
                at = pl.ds(pl.multiple_of(place, cap), cap)
                h_s[at, :] = got[o * cap : (o + 1) * cap, :width] * (1.0 / SCALE)
                f_s[at, :] = got[o * cap : (o + 1) * cap, width:]
    turned = f_s[...].T
    live[...] = turned[GROUPS : GROUPS + 8, 0:part]
    z_s[0:GROUPS, :] = turned[0:GROUPS, :].astype(I32)
    spot = slice(m * part, (m + 1) * part)
    z_s[GROUPS : GROUPS * STEPS, :] = jnp.concatenate(
        [g[0 : GROUPS * (STEPS - 1), spot].astype(I32) for g in given], 1
    )
    iota = lax.broadcasted_iota(I32, (CLASSES, rows), 0)
    for step in range(STEPS):
        for g in range(GROUPS):
            row = step * GROUPS + g
            hot = jnp.broadcast_to(z_s[row : row + 1, :], (CLASSES, rows)) == iota
            oh_s[g * CLASSES : (g + 1) * CLASSES, step * rows : (step + 1) * rows] = jnp.where(
                hot, 1.0, 0.0
            ).astype(BF16)
    dims = (((0,), (0,)), ((), ()))
    g_s[...] = lax.dot_general(
        oh_s[...], w_s[...], dims, preferred_element_type=F32
    ) + acts[m].astype(F32)
    keep = jnp.broadcast_to(f_s[:, GROUPS : GROUPS + 1], (rows, width)) > 0
    for step in range(STEPS):
        h = h_s[...]
        gates = g_s[step * rows : (step + 1) * rows, :] + jnp.dot(
            h.astype(BF16), wd_s[...], preferred_element_type=F32
        )
        reset = jax.nn.sigmoid(gates[:, :width])
        cand = jnp.tanh(reset * gates[:, width : 2 * width])
        update = jax.nn.sigmoid(gates[:, 2 * width :] - 1.0)
        h = update * cand + (1.0 - update) * h
        h_s[...] = h
        shown = jnp.where(keep, h, jnp.zeros_like(h)).astype(BF16)
        for k in range(nx):
            outs[k][step] = shown[k * part : (k + 1) * part, :]


def prior_kernel(nx, m, idx, known, live, wp_s, *rest):
    parts = rest[:nx]
    states, logp, st_s, out_sems = rest[-4:]
    ix, chip = idx[0], idx[1]
    width = parts[0].shape[2]
    count = parts[0].shape[1]
    for k in range(nx):
        at = pl.multiple_of((ix ^ k) * width, width)
        st_s[:, :, pl.ds(at, width)] = jnp.transpose(parts[k][...], (1, 0, 2))
    outgo = []
    run = count // nx
    for a in range(nx):
        outgo.append(
            pltpu.make_async_copy(
                st_s.at[pl.ds(a * run, run)], states.at[a, chip ^ m], out_sems.at[a]
            )
        )
    for copy in outgo:
        copy.start()
    logits = jnp.zeros((STEPS * count, wp_s.shape[1]), F32)
    for k in range(nx):
        at = pl.multiple_of((ix ^ k) * width, width)
        part = parts[k][...].reshape(STEPS * count, width)
        logits = logits + jnp.dot(part, wp_s[pl.ds(at, width), :], preferred_element_type=F32)
    turned = logits.T
    spot = slice(m * count, (m + 1) * count)
    z = jnp.concatenate(
        [known[t * GROUPS : (t + 1) * GROUPS, spot].astype(I32) for t in range(STEPS)], 1
    )
    alive = jnp.concatenate([live[0:1, :]] * STEPS, 1) > 0
    iota = lax.broadcasted_iota(I32, (CLASSES, STEPS * count), 0)
    for g in range(GROUPS):
        own = turned[g * CLASSES : (g + 1) * CLASSES, :]
        total = jnp.log(jnp.sum(jnp.exp(own), 0, keepdims=True))
        hot = jnp.broadcast_to(z[g : g + 1, :], own.shape) == iota
        picked = jnp.sum(jnp.where(hot, own, jnp.zeros_like(own)), 0, keepdims=True)
        logp[g : g + 1, :] = jnp.where(alive, picked - total, jnp.zeros_like(total))
    for copy in outgo:
        copy.wait()


def order_logp(chip, chips, run, logps, out):
    slots = out.shape[2]
    part = slots // chips
    order = slot_map(chip, chips, run, (slots, slots), 1)
    order = jnp.where(order, 1.0, 0.0).astype(BF16)
    for step in range(STEPS):
        value = jnp.concatenate([p[:, step * part : (step + 1) * part] for p in logps], 1)
        total = jnp.zeros(value.shape, F32)
        for _ in range(3):
            piece = value.astype(BF16)
            total = total + jnp.dot(piece, order, preferred_element_type=F32)
            value = value - piece.astype(F32)
        out[step] = total


def last_prior_kernel(chips, nx, m, run, idx, known, live, wp_s, *rest):
    logps, out, (st_s, logp, out_sems) = rest[nx : nx + m], rest[-4], rest[-3:]
    states = rest[-5]
    prior_kernel(nx, m, idx, known, live, wp_s, *rest[:nx], states, logp, st_s, out_sems)
    order_logp(idx[1], chips, run, list(logps) + [logp], out)


def fast_on_device(nx, ny):
    def on_device(
        replay_deter,
        replay_stoch,
        send_rows,
        send_counts,
        actions,
        samples,
        w_stoch,
        w_deter,
        act_table,
        w_prior,
    ):
        peers, cap = send_rows.shape
        slots = peers * cap
        deter = replay_deter.shape[1]
        blocks = w_deter.shape[0]
        width = deter // blocks
        cols = 3 * width
        chips = ny // 2
        part = nx * 2 * cap
        rows = nx * part
        lined = width + LANES
        ix = lax.axis_index("gx").astype(I32)
        iy = lax.axis_index("gy").astype(I32)
        idx = jnp.stack([ix, lax.shift_right_logical(iy, 1), iy & 1])
        ring = [(a, (a + 2) % ny) for a in range(ny)]
        partner = swap_pairs(ny, 1)

        def call(kernel, out_shape, ins, outs, scratch=(), mib=16, flops=0, **kwargs):
            def run(*args):
                return pl.pallas_call(
                    kernel,
                    out_shape=out_shape,
                    in_specs=ins,
                    out_specs=outs,
                    scratch_shapes=scratch,
                    compiler_params=params(mib),
                    cost_estimate=pl.CostEstimate(
                        flops=flops, transcendentals=0, bytes_accessed=2**20
                    ),
                    **kwargs,
                )(*args)

            return run

        srows, drows, prows = w_stoch.shape[0], w_deter.shape[1], w_prior.shape[0]
        wide = w_prior.shape[1] // nx
        own = call(
            weights_kernel,
            [
                jax.ShapeDtypeStruct((srows, cols), BF16),
                jax.ShapeDtypeStruct((drows, cols), BF16),
                jax.ShapeDtypeStruct((prows, wide), BF16),
            ],
            [SMEM, HBM, HBM, HBM],
            [VMEM] * 3,
            [pltpu.SemaphoreType.DMA((3,))],
        )(idx, *(pltpu.with_memory_space_constraint(w, pltpu.HBM) for w in (w_stoch, w_deter, w_prior)))
        stops = {}
        for name, shard in zip("sdp", own):
            stops[name] = [shard]
            for _ in range(1, chips):
                stops[name].append(lax.ppermute(stops[name][-1], "gy", ring))
        pieces = {}
        for name in "sd":
            pieces[name] = []
            for piece in stops[name]:
                pieces[name] += [piece, lax.ppermute(piece, "gy", partner)]
        column = call(
            functools.partial(column_kernel, chips, prows),
            jax.ShapeDtypeStruct((chips * prows, wide), BF16),
            [SMEM] + [VMEM] * chips,
            VMEM,
        )(idx, *stops["p"])
        priors = []
        for k in range(nx):
            piece = lax.ppermute(column, "gx", swap_pairs(nx, k)) if k else column
            priors += [piece, lax.ppermute(piece, "gy", partner)]

        stoch = jnp.transpose(replay_stoch)
        samp = jnp.transpose(samples, (1, 2, 0)).reshape(-1, slots)
        acts = jnp.transpose(actions)
        *held, known = call(
            functools.partial(pack_kernel, chips, nx, cap),
            [jax.ShapeDtypeStruct((slots // 2, lined), I16)] * (2 * nx)
            + [jax.ShapeDtypeStruct((samp.shape[0] + 16, slots), I16)],
            [SMEM] * 3 + [VMEM] * 4,
            [VMEM] * (2 * nx + 1),
            [
                pltpu.VMEM((slots, deter), F32),
                pltpu.VMEM((slots, LANES), F32),
                pltpu.VMEM((slots, replay_deter.shape[0]), F32),
            ],
        )(idx, jnp.transpose(send_rows), send_counts, replay_deter, stoch, samp, acts)
        for k in range(nx):
            for l in range(2):
                if k or l:
                    pairs = [
                        (a * ny + b, (a ^ k) * ny + (b ^ l)) for a in range(nx) for b in range(ny)
                    ]
                    n = k * 2 + l
                    held[n] = lax.ppermute(held[n], ("gx", "gy"), pairs)
        given = [known]
        for k in range(1, nx):
            given.append(lax.ppermute(known, "gx", swap_pairs(nx, k)))
        starts = call(
            functools.partial(fold_kernel, chips, nx * cap),
            [jax.ShapeDtypeStruct((2 * nx, nx * cap, lined), I16)] * chips,
            [VMEM] * (2 * nx),
            [VMEM] * chips,
        )(*held)
        starts = list(starts)
        for m in range(1, chips):
            starts[m] = lax.ppermute(starts[m], "gy", swap_pairs(ny, 2 * m))
        placed = []
        early = 2 * chips - 2
        for first, end in ((0, early), (early, 2 * chips)):
            some = pieces["s"][first:end] + pieces["d"][first:end]
            placed = call(
                functools.partial(place_kernel, chips, (srows, drows), first, len(placed)),
                [
                    jax.ShapeDtypeStruct((ny * srows, cols), BF16),
                    jax.ShapeDtypeStruct((ny * drows, cols), BF16),
                ],
                [SMEM] + [VMEM] * (len(some) + len(placed)),
                [VMEM] * 2,
                input_output_aliases={len(some) + 1 + n: n for n in range(len(placed))},
            )(idx, *some, *placed)
        w_all, wd_all = placed

        acts_all = call(
            functools.partial(acts_kernel, chips, rows, nx),
            jax.ShapeDtypeStruct((chips, STEPS * rows, cols), BF16),
            [SMEM] + [VMEM] * (1 + nx),
            VMEM,
            [
                pltpu.VMEM((CLASSES, cols), BF16),
                pltpu.VMEM((chips, 8, rows), I32),
                pltpu.VMEM((CLASSES, STEPS * rows), BF16),
            ],
        )(idx, act_table, *given)
        parts = []
        for m in range(chips):
            *outs, live = call(
                functools.partial(gru_kernel, rows, cap, nx, m),
                [jax.ShapeDtypeStruct((STEPS, part, width), BF16)] * nx
                + [jax.ShapeDtypeStruct((8, part), F32)],
                [SMEM] + [VMEM] * (4 + nx),
                [VMEM] * (nx + 1),
                [
                    pltpu.VMEM((GROUPS * CLASSES, STEPS * rows), BF16),
                    pltpu.VMEM((STEPS * rows, cols), F32),
                    pltpu.VMEM((rows, width), F32),
                    pltpu.VMEM((rows, LANES), F32),
                    pltpu.VMEM((GROUPS * STEPS, rows), I32),
                ],
                flops=2 * STEPS * rows * (GROUPS * CLASSES + width) * cols,
            )(idx, starts[m], acts_all, w_all, wd_all, *given)
            got = [outs[0]]
            for k in range(1, nx):
                got.append(lax.ppermute(outs[k], "gx", swap_pairs(nx, k)))
            parts.append((live, got))

        wp_all = call(
            functools.partial(prior_weights_kernel, chips, nx, prows),
            jax.ShapeDtypeStruct((deter, GROUPS * CLASSES), BF16),
            [SMEM] + [VMEM] * (2 * nx),
            VMEM,
        )(idx, *priors)

        shape = (nx, chips, 2 * cap, STEPS, deter)
        states = []
        logps = []
        for m in range(chips):
            live, got = parts[m]
            last = m + 1 == chips
            kernel = functools.partial(prior_kernel, nx, m)
            logp_shape = (GROUPS, STEPS * part)
            scratch = [pltpu.VMEM((part, STEPS, deter), BF16), pltpu.SemaphoreType.DMA((nx,))]
            if last:
                kernel = functools.partial(last_prior_kernel, chips, nx, m, 2 * cap)
                scratch.insert(1, pltpu.VMEM(logp_shape, F32))
                logp_shape = (STEPS, GROUPS, slots)
            more = logps if last else []
            filled, logp = call(
                kernel,
                [jax.ShapeDtypeStruct(shape, BF16), jax.ShapeDtypeStruct(logp_shape, F32)],
                [SMEM] + [VMEM] * (3 + nx + len(more)) + [ANY] * len(states),
                [ANY, VMEM],
                scratch,
                flops=2 * STEPS * part * deter * GROUPS * CLASSES,
                input_output_aliases={4 + nx + len(more): 0} if states else {},
            )(idx, known, live, wp_all, *got, *more, *states)
            states = [filled]
            logps.append(logp)
        return (filled.reshape(slots, STEPS, deter), jnp.transpose(logp, (2, 0, 1)))

    return on_device


def ring_gather(shard, count, index):
    chips = count // 2
    chip, core = index // 2, index % 2
    full = jnp.zeros((count,) + shard.shape, shard.dtype)
    piece = shard
    for hop in range(chips):
        if hop:
            piece = lax.ppermute(piece, "gy", [(a, (a + 2) % count) for a in range(count)])
        other = lax.ppermute(piece, "gy", swap_pairs(count, 1))
        place = lax.rem(chip + chips - hop, chips) * 2
        full = lax.dynamic_update_index_in_dim(full, piece, place + core, 0)
        full = lax.dynamic_update_index_in_dim(full, other, place + 1 - core, 0)
    return full


def one_hot(values, count):
    hot = values[..., None] == jnp.arange(count, dtype=jnp.int32)
    return hot.reshape(values.shape[0], -1).astype(jnp.bfloat16)


def plain_on_device(nx, ny):
    def on_device(
        replay_deter,
        replay_stoch,
        send_rows,
        send_counts,
        actions,
        samples,
        w_stoch,
        w_deter,
        act_table,
        w_prior,
    ):
        peers, cap = send_rows.shape
        slots = peers * cap
        deter = replay_deter.shape[1]
        blocks = w_deter.shape[0]
        assert blocks == nx
        width = deter // blocks
        cols = 3 * width
        ix = lax.axis_index("gx")
        iy = lax.axis_index("gy")

        ws = lax.dynamic_slice_in_dim(w_stoch, ix * cols, cols, 1)
        wd = lax.dynamic_index_in_dim(w_deter, ix, 0, keepdims=False)
        wa = lax.dynamic_slice_in_dim(act_table, ix * cols, cols, 1)
        ws = ring_gather(ws, ny, iy).reshape(-1, cols)
        wd = ring_gather(wd, ny, iy).reshape(-1, cols)

        picks = send_rows.reshape(slots)
        start = replay_deter[picks].astype(jnp.float16).reshape(nx, ny, cap, blocks, width)
        mine = jnp.zeros((nx, ny, nx, cap, width), jnp.float16)
        for k in range(nx):
            part = lax.dynamic_index_in_dim(start, ix ^ k, 3, keepdims=False)
            if k:
                part = lax.ppermute(part, "gx", swap_pairs(nx, k))
            mine = lax.dynamic_update_index_in_dim(mine, part, ix ^ k, 2)
        rows = jnp.zeros((nx, nx, ny, cap, width), jnp.float16)
        for k in range(ny):
            part = lax.dynamic_index_in_dim(mine, iy ^ k, 1, keepdims=False)
            if k:
                part = lax.ppermute(part, "gy", swap_pairs(ny, k))
            rows = lax.dynamic_update_index_in_dim(rows, part, iy ^ k, 2)
        state = rows.reshape(nx * slots, width).astype(jnp.float32)

        first = replay_stoch[picks].reshape(nx, ny, cap * GROUPS)
        note = jnp.concatenate([first, send_counts[0].reshape(nx, ny, 1)], 2)
        note = jnp.transpose(note, (1, 0, 2)).astype(jnp.bfloat16)
        note = jnp.broadcast_to(note[None], (nx,) + note.shape).reshape(peers, nx, -1)
        note = lax.all_to_all(note, ("gx", "gy"), split_axis=0, concat_axis=0, tiled=True)
        note = note.astype(jnp.int32)
        first = jnp.transpose(note[:, :, : cap * GROUPS], (1, 0, 2)).reshape(nx * slots, GROUPS)
        counts = lax.dynamic_index_in_dim(note, ix, 1, keepdims=False)[:, cap * GROUPS]
        live = (jnp.arange(cap, dtype=jnp.int32)[None, :] < counts[:, None]).reshape(slots)

        known = jnp.concatenate([samples[:, : STEPS - 1].reshape(slots, -1), actions], 1)
        given = jnp.zeros((nx,) + known.shape, known.dtype)
        for k in range(nx):
            part = lax.ppermute(known, "gx", swap_pairs(nx, k)) if k else known
            given = lax.dynamic_update_index_in_dim(given, part, ix ^ k, 0)
        given = given.reshape(nx * slots, -1)

        wp = ring_gather(w_prior, ny, iy).reshape(deter, -1)

        log_prob = []
        states = []
        for step in range(STEPS):
            z = first if step == 0 else given[:, GROUPS * (step - 1) : GROUPS * step]
            act = given[:, GROUPS * (STEPS - 1) + step]
            gates = (
                jnp.dot(one_hot(z, CLASSES), ws, preferred_element_type=jnp.float32)
                + jnp.dot(
                    one_hot(act, act_table.shape[0]), wa, preferred_element_type=jnp.float32
                )
                + jnp.dot(state.astype(jnp.bfloat16), wd, preferred_element_type=jnp.float32)
            )
            reset = jax.nn.sigmoid(gates[:, :width])
            cand = jnp.tanh(reset * gates[:, width : 2 * width])
            update = jax.nn.sigmoid(gates[:, 2 * width :] - 1.0)
            state = update * cand + (1.0 - update) * state
            out = state.astype(jnp.bfloat16).reshape(nx, slots, width)
            whole = jnp.zeros((slots, deter), jnp.bfloat16)
            for k in range(nx):
                part = lax.dynamic_index_in_dim(out, ix ^ k, 0, keepdims=False)
                if k:
                    part = lax.ppermute(part, "gx", swap_pairs(nx, k))
                whole = lax.dynamic_update_slice_in_dim(whole, part, (ix ^ k) * width, 1)
            whole = jnp.where(live[:, None], whole, jnp.zeros_like(whole))
            states.append(whole)
            logits = jnp.dot(whole, wp, preferred_element_type=jnp.float32)
            logits = logits.reshape(slots, GROUPS, CLASSES)
            totals = jnp.log(jnp.sum(jnp.exp(logits), -1))
            hits = samples[:, step, :, None] == jnp.arange(CLASSES, dtype=jnp.int32)
            picked = jnp.sum(jnp.where(hits, logits, jnp.zeros_like(logits)), -1)
            log_prob.append(jnp.where(live[:, None], picked - totals, jnp.zeros_like(totals)))
        return (jnp.stack(states, 1), jnp.stack(log_prob, 1))

    return on_device


def solution(mesh):
    nx, ny = mesh.shape["gx"], mesh.shape["gy"]

    def on_device(*args):
        if args[2].shape[1] % 8 == 0 and ny == 8:
            return fast_on_device(nx, ny)(*args)
        return plain_on_device(nx, ny)(*args)

    in_specs = (
        P(("gx", "gy"), None),
        P(("gx", "gy"), None),
        P(("gx", "gy"), None),
        P(("gx", "gy"), None),
        P(("gx", "gy"), None),
        P(("gx", "gy"), None, None),
        P("gy", None),
        P(None, "gy", None),
        P(),
        P("gy", None),
    )
    out_specs = (P(("gx", "gy"), None, None), P(("gx", "gy"), None, None))
    return jax.shard_map(
        on_device, mesh=mesh, in_specs=in_specs, out_specs=out_specs, check_vma=False
    )
```
